16 devices in a mesh: dp: 2 (over y, z), tp: 8 (over x, core).
Axes of the slice: x: 4, y: 2, z: 1, core: 2. Of those that a mesh axis runs over, the one named last changes fastest.
The devices are a block of a 4x4x8 slice.
Arguments:
- hidden: bfloat16 [256, 5120], P('dp'), parts along dimension 0
- positions: int32 [256], P('dp'), parts along dimension 0
- k_cache: bfloat16 [2, 256, 64, 8, 128], P(None, 'dp', None, 'tp'), parts along dimension 1
- v_cache: bfloat16 [2, 256, 64, 8, 128], P(None, 'dp', None, 'tp'), parts along dimension 1
- attn_norm: bfloat16 [2, 5120], replicated
- w_query: bfloat16 [2, 5120, 4096], P(None, None, 'tp')
- w_key: bfloat16 [2, 5120, 1024], P(None, None, 'tp')
- w_value: bfloat16 [2, 5120, 1024], P(None, None, 'tp')
- w_out: bfloat16 [2, 4096, 5120], P(None, 'tp')
- mlp_norm: bfloat16 [2, 5120], replicated
- w_gate: bfloat16 [2, 5120, 14336], P(None, None, 'tp')
- w_up: bfloat16 [2, 5120, 14336], P(None, None, 'tp')
- w_down: bfloat16 [2, 14336, 5120], P(None, 'tp')
Outputs:
- output 1: bfloat16 [256, 5120], P('dp'), parts along dimension 0
- output 2: bfloat16 [2, 256, 64, 8, 128], P(None, 'dp', None, 'tp'), parts along dimension 1
- output 3: bfloat16 [2, 256, 64, 8, 128], P(None, 'dp', None, 'tp'), parts along dimension 1
There are 2 independent parts. The reference program is written for one: setup_inputs(seed, part) draws one part's arguments, and reference() takes and returns one part's arrays. A program takes and returns all parts, laid end to end along the dimension named above; an argument that names none is the same for every part.
All inputs are finite; a program needn't handle non-finite values.
Results may differ from the reference program's by a relative error of at most 0.02.
Values are sent between devices in bfloat16 or wider.
A program may use at most 768 MiB of HBM per device.

```python
import math
import jax
import jax.numpy as jnp
from jax import lax

LAYERS = 2
BATCH = 128
SEQ = 64
D = 5120
HEADS = 32
KV_HEADS = 8
HEAD = 128
FF = 14336


def normal_weight(rng_key, shape, scale):
    return (jax.random.normal(rng_key, shape, jnp.float32) * scale).astype(jnp.bfloat16)


def setup_inputs(seed: int = 0, part: int = 0) -> dict:
    base_key = jax.random.key(seed)
    shared_keys = jax.random.split(base_key, 9)
    part_keys = jax.random.split(jax.random.fold_in(base_key, part), 5)
    cache_shape = (LAYERS, BATCH, SEQ, KV_HEADS, HEAD)
    drawn_pos = jax.random.randint(part_keys[1], (BATCH,), SEQ // 8, SEQ, dtype=jnp.int32)
    drawn_pos = drawn_pos.at[0].set(SEQ - 1).at[1].set(SEQ // 8)
    return dict(
        hidden=normal_weight(part_keys[0], (BATCH, D), 1.0),
        positions=jax.random.permutation(part_keys[2], drawn_pos),
        k_cache=normal_weight(part_keys[3], cache_shape, 1.0),
        v_cache=normal_weight(part_keys[4], cache_shape, 1.0),
        attn_norm=(1.0 + 0.3 * jax.random.normal(shared_keys[0], (LAYERS, D), jnp.float32)).astype(jnp.bfloat16),
        w_query=normal_weight(shared_keys[1], (LAYERS, D, HEADS * HEAD), D ** -0.5),
        w_key=normal_weight(shared_keys[2], (LAYERS, D, KV_HEADS * HEAD), 1.5 * D ** -0.5),
        w_value=normal_weight(shared_keys[3], (LAYERS, D, KV_HEADS * HEAD), 1.5 * D ** -0.5),
        w_out=normal_weight(shared_keys[4], (LAYERS, HEADS * HEAD, D), 0.5 * (SEQ / (HEADS * HEAD)) ** 0.5),
        mlp_norm=(1.0 + 0.3 * jax.random.normal(shared_keys[5], (LAYERS, D), jnp.float32)).astype(jnp.bfloat16),
        w_gate=normal_weight(shared_keys[6], (LAYERS, D, FF), D ** -0.5),
        w_up=normal_weight(shared_keys[7], (LAYERS, D, FF), D ** -0.5),
        w_down=normal_weight(shared_keys[8], (LAYERS, FF, D), 1.5 * FF ** -0.5),
    )


def rms_norm(hidden, weight):
    hidden_f32 = hidden.astype(jnp.float32)
    mean_sq = jnp.mean(hidden_f32 * hidden_f32, axis=-1, keepdims=True)
    return (hidden_f32 * lax.rsqrt(mean_sq + 1e-5) * weight.astype(jnp.float32)).astype(jnp.bfloat16)


def rope_tables(positions, head_dim):
    half_dim = head_dim // 2
    inv_freq = jnp.power(500000.0, -jnp.arange(half_dim, dtype=jnp.float32) * (2.0 / head_dim))
    wavelen = (2.0 * math.pi) / inv_freq
    smooth = (8192.0 / wavelen - 1.0) / 3.0
    blended = (1.0 - smooth) * inv_freq / 8.0 + smooth * inv_freq
    scaled = jnp.where(wavelen < 2048.0, inv_freq, jnp.where(wavelen > 8192.0, inv_freq / 8.0, blended))
    angles = positions.astype(jnp.float32)[:, None] * scaled[None, :]
    return jnp.cos(angles), jnp.sin(angles)


def apply_rope(vectors, cos_tab, sin_tab):
    half_dim = vectors.shape[-1] // 2
    vec_f32 = vectors.astype(jnp.float32)
    first = vec_f32[..., :half_dim]
    second = vec_f32[..., half_dim:]
    cos_b = cos_tab[:, None, :]
    sin_b = sin_tab[:, None, :]
    return jnp.concatenate([first * cos_b - second * sin_b, second * cos_b + first * sin_b], axis=-1).astype(jnp.bfloat16)


def attend(query, k_all, v_all, visible):
    scores = jnp.einsum('bkgd,bskd->bkgs', query.astype(jnp.float32), k_all.astype(jnp.float32)) * (query.shape[-1] ** -0.5)
    scores = jnp.where(visible, scores, -jnp.inf)
    prob_rows = jax.nn.softmax(scores, axis=-1).astype(jnp.bfloat16)
    attn_out = jnp.einsum('bkgs,bskd->bkgd', prob_rows.astype(jnp.float32), v_all.astype(jnp.float32))
    return attn_out.astype(jnp.bfloat16)


def reference(hidden, positions, k_cache, v_cache, attn_norm, w_query, w_key, w_value, w_out, mlp_norm, w_gate, w_up, w_down):
    group = HEADS // KV_HEADS
    cos_tab, sin_tab = rope_tables(positions, HEAD)
    seq_ids = jnp.arange(SEQ)
    at_pos = (seq_ids[None, :] == positions[:, None])[:, :, None, None]
    visible = (seq_ids[None, :] <= positions[:, None])[:, None, None, :]

    def layer_step(state, layer_args):
        norm_attn, wq_layer, wk_layer, wv_layer, wo_layer, norm_mlp, wg_layer, wu_layer, wd_layer, k_layer, v_layer = layer_args
        normed = rms_norm(state, norm_attn)
        query = jnp.dot(normed, wq_layer, preferred_element_type=jnp.float32).astype(jnp.bfloat16)
        key_new = jnp.dot(normed, wk_layer, preferred_element_type=jnp.float32).astype(jnp.bfloat16)
        value_new = jnp.dot(normed, wv_layer, preferred_element_type=jnp.float32).astype(jnp.bfloat16)
        query = apply_rope(query.reshape(BATCH, HEADS, HEAD), cos_tab, sin_tab)
        key_new = apply_rope(key_new.reshape(BATCH, KV_HEADS, HEAD), cos_tab, sin_tab)
        value_new = value_new.reshape(BATCH, KV_HEADS, HEAD)
        k_layer = jnp.where(at_pos, key_new[:, None], k_layer)
        v_layer = jnp.where(at_pos, value_new[:, None], v_layer)
        attended = attend(query.reshape(BATCH, KV_HEADS, group, HEAD), k_layer, v_layer, visible)
        mixed = jnp.dot(attended.reshape(BATCH, HEADS * HEAD), wo_layer, preferred_element_type=jnp.float32)
        state = state + mixed.astype(jnp.bfloat16)
        normed = rms_norm(state, norm_mlp)
        gate_proj = jnp.dot(normed, wg_layer, preferred_element_type=jnp.float32).astype(jnp.bfloat16)
        up_proj = jnp.dot(normed, wu_layer, preferred_element_type=jnp.float32).astype(jnp.bfloat16)
        activated = (jax.nn.silu(gate_proj.astype(jnp.float32)) * up_proj.astype(jnp.float32)).astype(jnp.bfloat16)
        state = state + jnp.dot(activated, wd_layer, preferred_element_type=jnp.float32).astype(jnp.bfloat16)
        return state, (k_layer, v_layer)

    stacked = (attn_norm, w_query, w_key, w_value, w_out, mlp_norm, w_gate, w_up, w_down, k_cache, v_cache)
    final, (k_out, v_out) = lax.scan(layer_step, hidden, stacked)
    return final, k_out, v_out
```

```python
import functools
import math
import jax
import jax.numpy as jnp
from jax import lax
from jax.experimental import pallas as pl
from jax.experimental.pallas import tpu as pltpu
from jax.sharding import PartitionSpec as P


def rms_norm(hidden, weight):
    hidden_f32 = hidden.astype(jnp.float32)
    mean_sq = jnp.mean(hidden_f32 * hidden_f32, axis=-1, keepdims=True)
    return (hidden_f32 * lax.rsqrt(mean_sq + 1e-5) * weight.astype(jnp.float32)).astype(jnp.bfloat16)


def rope_tables(positions, head_dim):
    half_dim = head_dim // 2
    inv_freq = jnp.power(500000.0, -jnp.arange(half_dim, dtype=jnp.float32) * (2.0 / head_dim))
    wavelen = (2.0 * math.pi) / inv_freq
    smooth = (8192.0 / wavelen - 1.0) / 3.0
    blended = (1.0 - smooth) * inv_freq / 8.0 + smooth * inv_freq
    scaled = jnp.where(wavelen < 2048.0, inv_freq, jnp.where(wavelen > 8192.0, inv_freq / 8.0, blended))
    angles = positions.astype(jnp.float32)[:, None] * scaled[None, :]
    return jnp.cos(angles), jnp.sin(angles)


def apply_rope(vectors, cos_tab, sin_tab):
    half_dim = vectors.shape[-1] // 2
    vec_f32 = vectors.astype(jnp.float32)
    first = vec_f32[..., :half_dim]
    second = vec_f32[..., half_dim:]
    cos_b = cos_tab[:, None, :]
    sin_b = sin_tab[:, None, :]
    return jnp.concatenate([first * cos_b - second * sin_b, second * cos_b + first * sin_b], axis=-1).astype(jnp.bfloat16)


def attend_split(query, k_old, v_old, key_new, value_new, before):
    score_scale = query.shape[-1] ** -0.5
    scores = jnp.einsum('bkgd,bskd->bkgs', query, k_old, preferred_element_type=jnp.float32) * score_scale
    scores = jnp.where(before, scores, -jnp.inf)
    score_new = jnp.einsum('clhe,cle->clh', query, key_new, preferred_element_type=jnp.float32) * score_scale
    row_peak = jnp.maximum(jnp.max(scores, axis=-1), score_new)
    weight_old = jnp.exp(scores - row_peak[..., None])
    weight_new = jnp.exp(score_new - row_peak)
    inv_total = 1.0 / (jnp.sum(weight_old, axis=-1) + weight_new)
    prob_old = (weight_old * inv_total[..., None]).astype(jnp.bfloat16)
    prob_new = (weight_new * inv_total).astype(jnp.bfloat16)
    attn_out = jnp.einsum('bkgs,bskd->bkgd', prob_old, v_old, preferred_element_type=jnp.float32)
    attn_out = attn_out + prob_new[..., None].astype(jnp.float32) * value_new[:, :, None, :].astype(jnp.float32)
    return attn_out.astype(jnp.bfloat16)


def attention_block(normed, wq_layer, wk_layer, wv_layer, k_old, v_old, cos_tab, sin_tab, before):
    batch_size = normed.shape[0]
    kv_heads = k_old.shape[2]
    head_dim = k_old.shape[3]
    q_heads = wq_layer.shape[1] // head_dim
    query = jnp.dot(normed, wq_layer, preferred_element_type=jnp.float32).astype(jnp.bfloat16)
    key_new = jnp.dot(normed, wk_layer, preferred_element_type=jnp.float32).astype(jnp.bfloat16)
    value_new = jnp.dot(normed, wv_layer, preferred_element_type=jnp.float32).astype(jnp.bfloat16)
    query = apply_rope(query.reshape(batch_size, q_heads, head_dim), cos_tab, sin_tab)
    key_new = apply_rope(key_new.reshape(batch_size, kv_heads, head_dim), cos_tab, sin_tab)
    value_new = value_new.reshape(batch_size, kv_heads, head_dim)
    attended = attend_split(query.reshape(batch_size, kv_heads, q_heads // kv_heads, head_dim), k_old, v_old, key_new, value_new, before)
    return attended.reshape(batch_size, q_heads * head_dim), key_new, value_new


PIECES = 4
TILE = 256


def mlp_kernel(layer, last, chips, attn_ref, res_ref, norm_mlp_ref, norm_next_ref, wo_hbm, wg_hbm, wu_hbm, wd_hbm, *rest):
    if last:
        out_ref, rest = rest[0], rest[1:]
    else:
        out_ref, own_ref, rest = rest[0], rest[1], rest[2:]
    (o_buf, g_buf, u_buf, d_buf, full, part, act, res, own_h, swap_in, summed, relay_in, relay_out, comb_in, direct_in,
     w_sem, io_sem, rs_send, rs_recv, ag_send, ag_recv) = rest
    rows, width = full.shape
    piece = width // PIECES
    half_rows = rows // 2
    own_rows = half_rows // chips
    half = width // 2
    me = lax.axis_index('tp')
    core = lax.rem(me, 2)
    chip = me // 2
    partner = me + 1 - 2 * core
    right = 2 * lax.rem(chip + 1, chips) + core
    left = 2 * lax.rem(chip + chips - 1, chips) + core
    row0 = pl.multiple_of(core * half_rows + chip * own_rows, own_rows)
    n_gate = g_buf.shape[0]

    def load_out(p):
        return pltpu.make_async_copy(wo_hbm.at[layer, :, pl.ds(p * piece, piece)], o_buf.at[p], w_sem.at[p])

    def load_down(p):
        return pltpu.make_async_copy(wd_hbm.at[layer, :, pl.ds(p * piece, piece)], d_buf.at[p], w_sem.at[PIECES + p])

    def load_gate(j):
        cols = pl.ds(pl.multiple_of(j * TILE, TILE), TILE)
        return pltpu.make_async_copy(wg_hbm.at[layer, :, cols], g_buf.at[j], w_sem.at[2 * PIECES + j])

    def load_up(j):
        cols = pl.ds(pl.multiple_of(j * TILE, TILE), TILE)
        return pltpu.make_async_copy(wu_hbm.at[layer, :, cols], u_buf.at[j], w_sem.at[2 * PIECES + n_gate + j])

    load_res = pltpu.make_async_copy(res_ref if last else res_ref.at[pl.ds(row0, own_rows)], res, io_sem.at[0])

    for p in range(PIECES):
        load_out(p).start()
    load_res.start()
    for j in range(n_gate):
        load_gate(j).start()
        load_up(j).start()
    for p in range(PIECES):
        load_down(p).start()

    barrier = pltpu.get_barrier_semaphore()
    for peer in (partner, right, left):
        pl.semaphore_signal(barrier, inc=1, device_id={'tp': peer}, device_id_type=pl.DeviceIdType.MESH)
    pl.semaphore_wait(barrier, 3)

    def remote(src, dst, send_sem, recv_sem, peer):
        return pltpu.make_async_remote_copy(src_ref=src, dst_ref=dst, send_sem=send_sem, recv_sem=recv_sem, device_id={'tp': peer}, device_id_type=pl.DeviceIdType.MESH)

    other_rows = pl.ds(pl.multiple_of((1 - core) * half_rows, half_rows), half_rows)
    my_rows = pl.ds(pl.multiple_of(core * half_rows, half_rows), half_rows)

    def block(offset):
        return pl.ds(pl.multiple_of(lax.rem(chip + offset, chips) * own_rows, own_rows), own_rows)

    def reduce_scatter(lhs_ref, w_buf, load):
        def swap(p):
            return remote(part.at[p, other_rows], swap_in.at[p], rs_send.at[0, p], rs_recv.at[0, p], partner)

        def relay(p):
            return remote(summed.at[p, block(2)], relay_in.at[p], rs_send.at[1, p], rs_recv.at[1, p], right if p % 2 == 0 else left)

        def direct(p):
            return remote(summed.at[p, block(chips - 1 if p % 2 == 0 else 1)], direct_in.at[p], rs_send.at[2, p], rs_recv.at[2, p], left if p % 2 == 0 else right)

        def combined(p):
            return remote(relay_out.at[p], comb_in.at[p], rs_send.at[3, p], rs_recv.at[3, p], right if p % 2 == 0 else left)

        def product(p):
            load(p).wait()
            for i in range(piece // TILE):
                cols = pl.ds(i * TILE, TILE)
                part[p, :, cols] = jnp.dot(lhs_ref[...], w_buf[p, :, cols], preferred_element_type=jnp.float32).astype(jnp.bfloat16)
            swap(p).start()

        def chip_sum(p):
            swap(p).wait_recv()
            summed[p] = (part[p, my_rows].astype(jnp.float32) + swap_in[p].astype(jnp.float32)).astype(jnp.bfloat16)
            relay(p).start()
            direct(p).start()

        def pass_on(p):
            relay(p).wait_recv()
            mine = summed[p, block(1 if p % 2 == 0 else chips - 1)]
            relay_out[p] = (mine.astype(jnp.float32) + relay_in[p].astype(jnp.float32)).astype(jnp.bfloat16)
            combined(p).start()

        product(0)
        product(1)
        chip_sum(0)
        product(2)
        chip_sum(1)
        product(3)
        pass_on(0)
        chip_sum(2)
        pass_on(1)
        chip_sum(3)
        pass_on(2)
        pass_on(3)
        sum_sq = jnp.zeros((own_rows, 1), jnp.float32)
        for p in range(PIECES):
            cols = pl.ds(p * piece, piece)
            direct(p).wait_recv()
            combined(p).wait_recv()
            total = summed[p, block(0)].astype(jnp.float32) + direct_in[p].astype(jnp.float32) + comb_in[p].astype(jnp.float32)
            new = res[:, cols].astype(jnp.float32) + total.astype(jnp.bfloat16).astype(jnp.float32)
            new = new.astype(jnp.bfloat16)
            res[:, cols] = new
            new = new.astype(jnp.float32)
            sum_sq = sum_sq + jnp.sum(new * new, axis=-1, keepdims=True)
        for p in range(PIECES):
            for copy in (swap(p), relay(p), direct(p), combined(p)):
                copy.wait_send()
        return sum_sq

    def normalize(sum_sq, norm_ref):
        scale = lax.rsqrt(sum_sq / width + 1e-5)
        for p in range(PIECES):
            cols = pl.ds(p * piece, piece)
            own_h[:, cols] = (res[:, cols].astype(jnp.float32) * scale * norm_ref[:, cols].astype(jnp.float32)).astype(jnp.bfloat16)

    def all_gather(src):
        first, second = pl.ds(0, half), pl.ds(half, half)

        def rows_of(offset, plane):
            return pl.ds(pl.multiple_of(plane * half_rows + lax.rem(chip + offset, chips) * own_rows, own_rows), own_rows)

        mine = rows_of(0, core)
        to_right = [(src.at[:, first], full.at[mine, first]), (src.at[:, second], full.at[mine, second])]
        to_left = [(src.at[:, second], full.at[mine, second]), (src.at[:, first], full.at[mine, first])]
        from_left, from_right, across = rows_of(chips - 1, core), rows_of(1, core), rows_of(2, core)
        arrived = [full.at[from_left, first], full.at[from_left, second], full.at[across, first],
                   full.at[from_right, second], full.at[from_right, first], full.at[across, second]]
        sends = [remote(*to_right[0], ag_send.at[0], ag_recv.at[0], right),
                 remote(*to_right[1], ag_send.at[1], ag_recv.at[1], right),
                 remote(arrived[0], arrived[0], ag_send.at[2], ag_recv.at[2], right),
                 remote(*to_left[0], ag_send.at[3], ag_recv.at[3], left),
                 remote(*to_left[1], ag_send.at[4], ag_recv.at[4], left),
                 remote(arrived[3], arrived[3], ag_send.at[5], ag_recv.at[5], left),
                 remote(src, full.at[mine], ag_send.at[6], ag_recv.at[6], partner)]
        forward = [remote(arrived[i], arrived[i], ag_send.at[7 + i], ag_recv.at[7 + i], partner) for i in range(6)]
        for i in (0, 3, 6, 1, 4):
            sends[i].start()
        full[mine, :] = src[...]
        sends[0].wait_recv()
        sends[2].start()
        forward[0].start()
        sends[3].wait_recv()
        sends[5].start()
        forward[3].start()
        for i in (1, 4, 2, 5):
            sends[i].wait_recv()
            forward[i].start()
        sends[6].wait_recv()
        for i in range(6):
            forward[i].wait_recv()
        for copy in sends + forward:
            copy.wait_send()

    load_res.wait()
    sum_sq = reduce_scatter(attn_ref, o_buf, load_out)
    normalize(sum_sq, norm_mlp_ref)
    all_gather(own_h)

    def gate_up(j, carry):
        load_gate(j).wait()
        load_up(j).wait()
        gate = jnp.dot(full[...], g_buf[j], preferred_element_type=jnp.float32).astype(jnp.bfloat16).astype(jnp.float32)
        up = jnp.dot(full[...], u_buf[j], preferred_element_type=jnp.float32).astype(jnp.bfloat16).astype(jnp.float32)
        act[:, pl.ds(pl.multiple_of(j * TILE, TILE), TILE)] = (gate * jax.nn.sigmoid(gate) * up).astype(jnp.bfloat16)
        return carry

    lax.fori_loop(0, n_gate, gate_up, 0)
    sum_sq = reduce_scatter(act, d_buf, load_down)
    if last:
        all_gather(res)
    else:
        normalize(sum_sq, norm_next_ref)
        own_ref[...] = res[...]
        all_gather(own_h)
    store = pltpu.make_async_copy(full, out_ref, io_sem.at[0])
    store.start()
    store.wait()


def mlp_call(layer, last, chips, attended, residual, norm_mlp, norm_next, w_out, w_gate, w_up, w_down):
    rows, inner = attended.shape
    width = w_gate.shape[1]
    ff = w_gate.shape[2]
    piece = width // PIECES
    own_rows = rows // 2 // chips
    bf16 = jnp.bfloat16
    vmem = pl.BlockSpec(memory_space=pltpu.VMEM)
    hbm = pl.BlockSpec(memory_space=pl.ANY)
    out_shape = [jax.ShapeDtypeStruct((rows, width), bf16)]
    out_specs = [hbm]
    if not last:
        out_shape.append(jax.ShapeDtypeStruct((own_rows, width), bf16))
        out_specs.append(vmem)
    scratch = [
        pltpu.VMEM((PIECES, inner, piece), bf16),
        pltpu.VMEM((ff // TILE, width, TILE), bf16),
        pltpu.VMEM((ff // TILE, width, TILE), bf16),
        pltpu.VMEM((PIECES, ff, piece), bf16),
        pltpu.VMEM((rows, width), bf16),
        pltpu.VMEM((PIECES, rows, piece), bf16),
        pltpu.VMEM((rows, ff), bf16),
        pltpu.VMEM((own_rows, width), bf16),
        pltpu.VMEM((own_rows, width), bf16),
        pltpu.VMEM((PIECES, rows // 2, piece), bf16),
        pltpu.VMEM((PIECES, rows // 2, piece), bf16),
        pltpu.VMEM((PIECES, own_rows, piece), bf16),
        pltpu.VMEM((PIECES, own_rows, piece), bf16),
        pltpu.VMEM((PIECES, own_rows, piece), bf16),
        pltpu.VMEM((PIECES, own_rows, piece), bf16),
        pltpu.SemaphoreType.DMA((2 * PIECES + 2 * (ff // TILE),)),
        pltpu.SemaphoreType.DMA((1,)),
        pltpu.SemaphoreType.DMA((4, PIECES)),
        pltpu.SemaphoreType.DMA((4, PIECES)),
        pltpu.SemaphoreType.DMA((13,)),
        pltpu.SemaphoreType.DMA((13,)),
    ]
    weights = inner * width + 3 * width * ff
    return pl.pallas_call(
        functools.partial(mlp_kernel, layer, last, chips),
        out_shape=out_shape,
        in_specs=[vmem, hbm, vmem, vmem, hbm, hbm, hbm, hbm],
        out_specs=out_specs,
        scratch_shapes=scratch,
        compiler_params=pltpu.CompilerParams(collective_id=layer, has_side_effects=True, vmem_limit_bytes=67043328),
        cost_estimate=pl.CostEstimate(flops=2 * rows * weights, bytes_accessed=2 * weights, transcendentals=rows * ff),
        name='mlp_layer',
    )(attended, residual, norm_mlp, norm_next, w_out, w_gate, w_up, w_down)


def write_rows(cache, rows, positions):
    at_pos = (jnp.arange(cache.shape[2])[None, :] == positions[:, None])[None, :, :, None, None]
    return jnp.where(at_pos, rows[:, :, None], cache)


def solution(mesh):
    row_spec = P('dp', None)
    pos_spec = P('dp')
    cache_spec = P(None, 'dp', None, 'tp', None)
    norm_spec = P(None, None)
    col_spec = P(None, None, 'tp')
    split_rows = P(None, 'tp', None)
    chips = mesh.shape['tp'] // 2

    def local_step(hidden, positions, k_cache, v_cache, attn_norm, w_query, w_key, w_value, w_out, mlp_norm, w_gate, w_up, w_down):
        cos_tab, sin_tab = rope_tables(positions, k_cache.shape[4])
        before = (jnp.arange(k_cache.shape[2])[None, :] < positions[:, None])[:, None, None, :]
        k_rows = []
        v_rows = []
        layers = k_cache.shape[0]
        normed, residual = rms_norm(hidden, attn_norm[0]), hidden
        for layer in range(layers):
            last = layer == layers - 1
            attended, key_new, value_new = attention_block(normed, w_query[layer], w_key[layer], w_value[layer], k_cache[layer], v_cache[layer], cos_tab, sin_tab, before)
            following = layer if last else layer + 1
            outs = mlp_call(layer, last, chips, attended, residual, mlp_norm[layer:layer + 1], attn_norm[following:following + 1], w_out, w_gate, w_up, w_down)
            if last:
                hidden = outs[0]
            else:
                normed, residual = outs
            k_rows.append(key_new)
            v_rows.append(value_new)
        k_out = write_rows(k_cache, jnp.stack(k_rows), positions)
        v_out = write_rows(v_cache, jnp.stack(v_rows), positions)
        return hidden, k_out, v_out

    return jax.shard_map(local_step, mesh=mesh, in_specs=(row_spec, pos_spec, cache_spec, cache_spec, norm_spec, col_spec, col_spec, col_spec, split_rows, norm_spec, col_spec, col_spec, split_rows), out_specs=(row_spec, cache_spec, cache_spec), check_vma=False)
```

```python
import functools
import math
import jax
import jax.numpy as jnp
from jax import lax
from jax.experimental import pallas as pl
from jax.experimental.pallas import tpu as pltpu
from jax.sharding import PartitionSpec as P


def rope_tables(positions, head_dim):
    half_dim = head_dim // 2
    inv_freq = jnp.power(500000.0, -jnp.arange(half_dim, dtype=jnp.float32) * (2.0 / head_dim))
    wavelen = (2.0 * math.pi) / inv_freq
    smooth = (8192.0 / wavelen - 1.0) / 3.0
    blended = (1.0 - smooth) * inv_freq / 8.0 + smooth * inv_freq
    scaled = jnp.where(wavelen < 2048.0, inv_freq, jnp.where(wavelen > 8192.0, inv_freq / 8.0, blended))
    angles = positions.astype(jnp.float32)[:, None] * scaled[None, :]
    return jnp.cos(angles), jnp.sin(angles)


def attention_kernel(layer, first, x_ref, norm_ref, pos_smem, pos_ref, cos_ref, sin_ref, wq_hbm, wk_hbm, wv_hbm, k_hbm, v_hbm, *rest):
    if not first:
        rest = rest[2:]
    (out_ref, k_out, v_out, wq_buf, wkv_buf, k_buf, v_buf, h_buf, q_buf, kv_buf, w_sem, in_sem, out_sem) = rest
    rows, width = x_ref.shape
    inner = wq_buf.shape[1]
    seq, dim = k_buf.shape[1], k_buf.shape[2]
    heads = inner // dim
    chunk = width // CHUNKS
    groups = rows // GROUP

    def load_weights(i):
        ks = pl.ds(i * chunk, chunk)
        return (pltpu.make_async_copy(wq_hbm.at[layer, ks], wq_buf.at[ks], w_sem.at[0, i]),
                pltpu.make_async_copy(wk_hbm.at[layer, ks], wkv_buf.at[ks, pl.ds(0, dim)], w_sem.at[1, i]),
                pltpu.make_async_copy(wv_hbm.at[layer, ks], wkv_buf.at[ks, pl.ds(dim, dim)], w_sem.at[2, i]))

    load_k = pltpu.make_async_copy(k_hbm.at[layer], k_buf, in_sem.at[0])
    load_v = pltpu.make_async_copy(v_hbm.at[layer], v_buf, in_sem.at[1])
    for i in range(CHUNKS):
        for copy in load_weights(i):
            copy.start()
    load_k.start()
    load_v.start()

    if first:
        sum_sq = jnp.zeros((rows, 1), jnp.float32)
        for i in range(CHUNKS):
            part = x_ref[:, pl.ds(i * chunk, chunk)].astype(jnp.float32)
            sum_sq = sum_sq + jnp.sum(part * part, axis=-1, keepdims=True)
        scale = lax.rsqrt(sum_sq / width + 1e-5)
        for i in range(CHUNKS):
            cols = pl.ds(i * chunk, chunk)
            h_buf[:, cols] = (x_ref[:, cols].astype(jnp.float32) * scale * norm_ref[:, cols].astype(jnp.float32)).astype(jnp.bfloat16)
        h_ref = h_buf
    else:
        h_ref = x_ref

    for i in range(CHUNKS):
        for copy in load_weights(i):
            copy.wait()
        ks = pl.ds(i * chunk, chunk)
        q_part = jnp.dot(h_ref[:, ks], wq_buf[ks, :], preferred_element_type=jnp.float32)
        kv_part = jnp.dot(h_ref[:, ks], wkv_buf[ks, :], preferred_element_type=jnp.float32)
        if i == 0:
            q_buf[...] = q_part
            kv_buf[...] = kv_part
        else:
            q_buf[...] += q_part
            kv_buf[...] += kv_part

    def rounded(value):
        return value.astype(jnp.bfloat16).astype(jnp.float32)

    def rope(vec):
        vec = rounded(vec)
        half = dim // 2
        swapped = jnp.concatenate([vec[:, half:], vec[:, :half]], axis=-1)
        return rounded(vec * cos_ref[...] + swapped * sin_ref[...])

    for j in range(heads):
        cols = pl.ds(j * dim, dim)
        q_buf[:, cols] = rope(q_buf[:, cols])
    kv_buf[:, pl.ds(0, dim)] = rope(kv_buf[:, pl.ds(0, dim)])
    kv_buf[:, pl.ds(dim, dim)] = rounded(kv_buf[:, pl.ds(dim, dim)])

    load_k.wait()
    load_v.wait()

    def store(g):
        part = pl.ds(pl.multiple_of(g * GROUP, GROUP), GROUP)
        return (pltpu.make_async_copy(k_buf.at[part], k_out.at[layer, part], out_sem.at[0, g]),
                pltpu.make_async_copy(v_buf.at[part], v_out.at[layer, part], out_sem.at[1, g]))

    def attend(g, carry):
        base = pl.multiple_of(g * GROUP, GROUP)
        fresh = kv_buf[pl.ds(base, GROUP), :]
        for i in range(GROUP):
            pos = pos_smem[base + i]
            top = pl.multiple_of((pos // ROWS) * ROWS, ROWS)
            here = lax.broadcasted_iota(jnp.int32, (ROWS, dim), 0) == pos - top
            for buf, off in ((k_buf, 0), (v_buf, dim)):
                old = buf[base + i, pl.ds(top, ROWS), :].astype(jnp.float32)
                new = jnp.broadcast_to(fresh[i:i + 1, off:off + dim], (ROWS, dim))
                buf[base + i, pl.ds(top, ROWS), :] = jnp.where(here, new, old).astype(jnp.bfloat16)
        block = pl.ds(base, GROUP)
        query = jnp.concatenate([q_buf[block, pl.ds(j * dim, dim)] for j in range(heads)], axis=0).astype(jnp.bfloat16)
        keys = k_buf[block].reshape(GROUP * seq, dim)
        values = v_buf[block].reshape(GROUP * seq, dim)
        scores = lax.dot_general(query, keys, (((1,), (1,)), ((), ())), preferred_element_type=jnp.float32) * (dim ** -0.5)
        shape = (heads * GROUP, GROUP * seq)
        start = lax.rem(lax.broadcasted_iota(jnp.int32, shape, 0), GROUP) * seq
        col = lax.broadcasted_iota(jnp.int32, shape, 1)
        upto = start + jnp.concatenate([pos_ref[block, :]] * heads, axis=0)
        scores = jnp.where((col >= start) & (col <= upto), scores, -jnp.inf)
        weight = jnp.exp(scores - jnp.max(scores, axis=-1, keepdims=True))
        prob = (weight * (1.0 / jnp.sum(weight, axis=-1, keepdims=True))).astype(jnp.bfloat16)
        mixed = jnp.dot(prob, values, preferred_element_type=jnp.float32)
        for j in range(heads):
            q_buf[block, pl.ds(j * dim, dim)] = mixed[j * GROUP:(j + 1) * GROUP]
        for copy in store(g):
            copy.start()
        return carry

    lax.fori_loop(0, groups, attend, 0)
    out_ref[...] = q_buf[...].astype(jnp.bfloat16)

    def drain(g, carry):
        for copy in store(g):
            copy.wait()
        return carry

    lax.fori_loop(0, groups, drain, 0)


CHUNKS = 4
GROUP = 8
ROWS = 16


def attention_call(layer, x, norm, positions, cos_tab, sin_tab, w_query, w_key, w_value, k_cache, v_cache, k_done, v_done):
    rows, width = x.shape
    inner = w_query.shape[2]
    seq, dim = k_cache.shape[2], k_cache.shape[3]
    bf16 = jnp.bfloat16
    first = k_done is None
    vmem = pl.BlockSpec(memory_space=pltpu.VMEM)
    hbm = pl.BlockSpec(memory_space=pltpu.HBM)
    smem = pl.BlockSpec(memory_space=pltpu.SMEM)
    args = [x, norm, positions, positions[:, None], cos_tab, sin_tab, w_query, w_key, w_value, k_cache, v_cache]
    specs = [vmem, vmem, smem, vmem, vmem, vmem, hbm, hbm, hbm, hbm, hbm]
    aliases = {}
    if not first:
        aliases = {len(args): 1, len(args) + 1: 2}
        args += [k_done, v_done]
        specs += [hbm, hbm]
    weights = width * (inner + 2 * dim)
    return pl.pallas_call(
        functools.partial(attention_kernel, layer, first),
        out_shape=[jax.ShapeDtypeStruct((rows, inner), bf16), jax.ShapeDtypeStruct(k_cache.shape, bf16), jax.ShapeDtypeStruct(v_cache.shape, bf16)],
        in_specs=specs,
        out_specs=[vmem, hbm, hbm],
        scratch_shapes=[
            pltpu.VMEM((width, inner), bf16),
            pltpu.VMEM((width, 2 * dim), bf16),
            pltpu.VMEM((rows, seq, dim), bf16),
            pltpu.VMEM((rows, seq, dim), bf16),
            pltpu.VMEM((rows, width), bf16),
            pltpu.VMEM((rows, inner), jnp.float32),
            pltpu.VMEM((rows, 2 * dim), jnp.float32),
            pltpu.SemaphoreType.DMA((3, CHUNKS)),
            pltpu.SemaphoreType.DMA((2,)),
            pltpu.SemaphoreType.DMA((2, rows // GROUP)),
        ],
        input_output_aliases=aliases,
        compiler_params=pltpu.CompilerParams(vmem_limit_bytes=67043328),
        cost_estimate=pl.CostEstimate(flops=2 * rows * weights, bytes_accessed=2 * weights, transcendentals=rows * seq),
        name='attention_layer',
    )(*args)


PIECES = 4
TILE = 256


def mlp_kernel(layer, last, chips, attn_ref, res_ref, norm_mlp_ref, norm_next_ref, wo_hbm, wg_hbm, wu_hbm, wd_hbm, *rest):
    if last:
        out_ref, rest = rest[0], rest[1:]
    else:
        out_ref, own_ref, rest = rest[0], rest[1], rest[2:]
    (o_buf, g_buf, u_buf, d_buf, full, part, act, res, own_h, swap_in, summed, owner_in,
     w_sem, io_sem, rs_send, rs_recv, ag_send, ag_recv) = rest
    rows, width = full.shape
    piece = width // PIECES
    half_rows = rows // 2
    own_rows = half_rows // chips
    half = width // 2
    me = lax.axis_index('tp')
    core = lax.rem(me, 2)
    chip = me // 2
    partner = me + 1 - 2 * core
    peers = [2 * lax.rem(chip + hop, chips) + core for hop in range(chips)]
    hops = tuple(sorted(range(1, chips), key=lambda hop: -min(hop, chips - hop)))
    row0 = pl.multiple_of(core * half_rows + chip * own_rows, own_rows)
    n_gate = g_buf.shape[0]

    def load_out(p):
        return pltpu.make_async_copy(wo_hbm.at[layer, :, pl.ds(p * piece, piece)], o_buf.at[p], w_sem.at[p])

    def load_down(p):
        return pltpu.make_async_copy(wd_hbm.at[layer, :, pl.ds(p * piece, piece)], d_buf.at[p], w_sem.at[PIECES + p])

    def load_gate(j):
        cols = pl.ds(pl.multiple_of(j * TILE, TILE), TILE)
        return pltpu.make_async_copy(wg_hbm.at[layer, :, cols], g_buf.at[j], w_sem.at[2 * PIECES + j])

    def load_up(j):
        cols = pl.ds(pl.multiple_of(j * TILE, TILE), TILE)
        return pltpu.make_async_copy(wu_hbm.at[layer, :, cols], u_buf.at[j], w_sem.at[2 * PIECES + n_gate + j])

    load_res = pltpu.make_async_copy(res_ref if last else res_ref.at[pl.ds(row0, own_rows)], res, io_sem.at[0])

    for p in range(PIECES):
        load_out(p).start()
    load_res.start()

    def start_gate_up():
        for j in range(n_gate):
            load_gate(j).start()
            load_up(j).start()

    barrier = pltpu.get_barrier_semaphore()
    for peer in [partner] + peers[1:]:
        pl.semaphore_signal(barrier, inc=1, device_id={'tp': peer}, device_id_type=pl.DeviceIdType.MESH)
    pl.semaphore_wait(barrier, chips)

    def remote(src, dst, send_sem, recv_sem, peer):
        return pltpu.make_async_remote_copy(src_ref=src, dst_ref=dst, send_sem=send_sem, recv_sem=recv_sem, device_id={'tp': peer}, device_id_type=pl.DeviceIdType.MESH)

    other_rows = pl.ds(pl.multiple_of((1 - core) * half_rows, half_rows), half_rows)
    my_rows = pl.ds(pl.multiple_of(core * half_rows, half_rows), half_rows)

    def block(offset):
        return pl.ds(pl.multiple_of(lax.rem(chip + offset, chips) * own_rows, own_rows), own_rows)

    def reduce_scatter(lhs_ref, w_buf, load, after_loads):
        def swap(p):
            return remote(part.at[p, other_rows], swap_in.at[p], rs_send.at[0, p], rs_recv.at[0, p], partner)

        def to_owner(p, hop):
            return remote(summed.at[p, block(hop)], owner_in.at[hop - 1, p], rs_send.at[hop, p], rs_recv.at[hop, p], peers[hop])

        def product(p):
            load(p).wait()
            for i in range(piece // TILE):
                cols = pl.ds(i * TILE, TILE)
                part[p, :, cols] = jnp.dot(lhs_ref[...], w_buf[p, :, cols], preferred_element_type=jnp.float32).astype(jnp.bfloat16)
            swap(p).start()

        def chip_sum(p):
            swap(p).wait_recv()
            summed[p] = (part[p, my_rows].astype(jnp.float32) + swap_in[p].astype(jnp.float32)).astype(jnp.bfloat16)
            for hop in hops:
                to_owner(p, hop).start()

        product(0)
        product(1)
        chip_sum(0)
        for p in range(2, PIECES):
            product(p)
            chip_sum(p - 1)
        after_loads()
        chip_sum(PIECES - 1)
        sum_sq = jnp.zeros((own_rows, 1), jnp.float32)
        for p in range(PIECES):
            cols = pl.ds(p * piece, piece)
            total = summed[p, block(0)].astype(jnp.float32)
            for hop in range(1, chips):
                to_owner(p, hop).wait_recv()
                total = total + owner_in[hop - 1, p].astype(jnp.float32)
            new = res[:, cols].astype(jnp.float32) + total.astype(jnp.bfloat16).astype(jnp.float32)
            new = new.astype(jnp.bfloat16)
            res[:, cols] = new
            new = new.astype(jnp.float32)
            sum_sq = sum_sq + jnp.sum(new * new, axis=-1, keepdims=True)
        for p in range(PIECES):
            swap(p).wait_send()
            for hop in range(1, chips):
                to_owner(p, hop).wait_send()
        return sum_sq

    def normalize(sum_sq, norm_ref):
        scale = lax.rsqrt(sum_sq / width + 1e-5)
        for p in range(PIECES):
            cols = pl.ds(p * piece, piece)
            own_h[:, cols] = (res[:, cols].astype(jnp.float32) * scale * norm_ref[:, cols].astype(jnp.float32)).astype(jnp.bfloat16)

    def all_gather(src):
        def rows_of(offset):
            return pl.ds(pl.multiple_of(core * half_rows + lax.rem(chip + offset, chips) * own_rows, own_rows), own_rows)

        mine = rows_of(0)
        sends = [remote(src, full.at[mine], ag_send.at[hop], ag_recv.at[hop], peers[hop] if hop else partner) for hop in range(chips)]
        forward = [None]
        for hop in range(1, chips):
            landed = full.at[rows_of(chips - hop)]
            forward.append(remote(landed, landed, ag_send.at[chips + hop - 1], ag_recv.at[chips + hop - 1], partner))
        for hop in hops + (0,):
            sends[hop].start()
        full[mine, :] = src[...]
        for hop in (1, chips - 1) + tuple(range(2, chips - 1)):
            sends[hop].wait_recv()
            forward[hop].start()
        sends[0].wait_recv()
        for hop in range(1, chips):
            forward[hop].wait_recv()
        for copy in sends + forward[1:]:
            copy.wait_send()

    load_res.wait()
    sum_sq = reduce_scatter(attn_ref, o_buf, load_out, start_gate_up)
    for p in range(PIECES):
        load_down(p).start()
    normalize(sum_sq, norm_mlp_ref)
    all_gather(own_h)

    def gate_up(j, carry):
        load_gate(j).wait()
        load_up(j).wait()
        gate = jnp.dot(full[...], g_buf[j], preferred_element_type=jnp.float32).astype(jnp.bfloat16).astype(jnp.float32)
        up = jnp.dot(full[...], u_buf[j], preferred_element_type=jnp.float32).astype(jnp.bfloat16).astype(jnp.float32)
        act[:, pl.ds(pl.multiple_of(j * TILE, TILE), TILE)] = (gate * jax.nn.sigmoid(gate) * up).astype(jnp.bfloat16)
        return carry

    lax.fori_loop(0, n_gate, gate_up, 0)
    sum_sq = reduce_scatter(act, d_buf, load_down, lambda: None)
    if last:
        all_gather(res)
    else:
        normalize(sum_sq, norm_next_ref)
        own_ref[...] = res[...]
        all_gather(own_h)
    store = pltpu.make_async_copy(full, out_ref, io_sem.at[0])
    store.start()
    store.wait()


def mlp_call(layer, last, chips, attended, residual, norm_mlp, norm_next, w_out, w_gate, w_up, w_down):
    rows, inner = attended.shape
    width = w_gate.shape[1]
    ff = w_gate.shape[2]
    piece = width // PIECES
    own_rows = rows // 2 // chips
    bf16 = jnp.bfloat16
    vmem = pl.BlockSpec(memory_space=pltpu.VMEM)
    hbm = pl.BlockSpec(memory_space=pltpu.HBM)
    out_shape = [jax.ShapeDtypeStruct((rows, width), bf16)]
    out_specs = [hbm]
    if not last:
        out_shape.append(jax.ShapeDtypeStruct((own_rows, width), bf16))
        out_specs.append(vmem)
    scratch = [
        pltpu.VMEM((PIECES, inner, piece), bf16),
        pltpu.VMEM((ff // TILE, width, TILE), bf16),
        pltpu.VMEM((ff // TILE, width, TILE), bf16),
        pltpu.VMEM((PIECES, ff, piece), bf16),
        pltpu.VMEM((rows, width), bf16),
        pltpu.VMEM((PIECES, rows, piece), bf16),
        pltpu.VMEM((rows, ff), bf16),
        pltpu.VMEM((own_rows, width), bf16),
        pltpu.VMEM((own_rows, width), bf16),
        pltpu.VMEM((PIECES, rows // 2, piece), bf16),
        pltpu.VMEM((PIECES, rows // 2, piece), bf16),
        pltpu.VMEM((chips - 1, PIECES, own_rows, piece), bf16),
        pltpu.SemaphoreType.DMA((2 * PIECES + 2 * (ff // TILE),)),
        pltpu.SemaphoreType.DMA((1,)),
        pltpu.SemaphoreType.DMA((chips, PIECES)),
        pltpu.SemaphoreType.DMA((chips, PIECES)),
        pltpu.SemaphoreType.DMA((2 * chips - 1,)),
        pltpu.SemaphoreType.DMA((2 * chips - 1,)),
    ]
    weights = inner * width + 3 * width * ff
    return pl.pallas_call(
        functools.partial(mlp_kernel, layer, last, chips),
        out_shape=out_shape,
        in_specs=[vmem, hbm, vmem, vmem, hbm, hbm, hbm, hbm],
        out_specs=out_specs,
        scratch_shapes=scratch,
        compiler_params=pltpu.CompilerParams(collective_id=layer, has_side_effects=True, vmem_limit_bytes=67043328),
        cost_estimate=pl.CostEstimate(flops=2 * rows * weights, bytes_accessed=2 * weights, transcendentals=rows * ff),
        name='mlp_layer',
    )(attended, residual, norm_mlp, norm_next, w_out, w_gate, w_up, w_down)


def solution(mesh):
    row_spec = P('dp', None)
    pos_spec = P('dp')
    cache_spec = P(None, 'dp', None, 'tp', None)
    norm_spec = P(None, None)
    col_spec = P(None, None, 'tp')
    split_rows = P(None, 'tp', None)
    chips = mesh.shape['tp'] // 2

    def local_step(hidden, positions, k_cache, v_cache, attn_norm, w_query, w_key, w_value, w_out, mlp_norm, w_gate, w_up, w_down):
        layers, batch, seq, kv_heads, dim = k_cache.shape
        cos_tab, sin_tab = rope_tables(positions, dim)
        cos_tab = jnp.concatenate([cos_tab, cos_tab], axis=-1)
        sin_tab = jnp.concatenate([-sin_tab, sin_tab], axis=-1)
        k_cache = k_cache.reshape(layers, batch, seq, dim)
        v_cache = v_cache.reshape(layers, batch, seq, dim)
        k_out = v_out = None
        stream = residual = hidden
        for layer in range(layers):
            last = layer == layers - 1
            attended, k_out, v_out = attention_call(layer, stream, attn_norm[layer:layer + 1], positions, cos_tab, sin_tab, w_query, w_key, w_value, k_cache, v_cache, k_out, v_out)
            following = layer if last else layer + 1
            outs = mlp_call(layer, last, chips, attended, residual, mlp_norm[layer:layer + 1], attn_norm[following:following + 1], w_out, w_gate, w_up, w_down)
            if last:
                hidden = outs[0]
            else:
                stream, residual = outs
        shape = (layers, batch, seq, kv_heads, dim)
        return hidden, k_out.reshape(shape), v_out.reshape(shape)

    return jax.shard_map(local_step, mesh=mesh, in_specs=(row_spec, pos_spec, cache_spec, cache_spec, norm_spec, col_spec, col_spec, col_spec, split_rows, norm_spec, col_spec, col_spec, split_rows), out_specs=(row_spec, cache_spec, cache_spec), check_vma=False)
```

```python
import functools
import math
import jax
import jax.numpy as jnp
from jax import lax
from jax.experimental import pallas as pl
from jax.experimental.pallas import tpu as pltpu
from jax.sharding import PartitionSpec as P


def rope_freqs(head_dim):
    half_dim = head_dim // 2
    inv_freq = jnp.power(500000.0, -jnp.arange(half_dim, dtype=jnp.float32) * (2.0 / head_dim))
    wavelen = (2.0 * math.pi) / inv_freq
    smooth = (8192.0 / wavelen - 1.0) / 3.0
    blended = (1.0 - smooth) * inv_freq / 8.0 + smooth * inv_freq
    scaled = jnp.where(wavelen < 2048.0, inv_freq, jnp.where(wavelen > 8192.0, inv_freq / 8.0, blended))
    return jnp.concatenate([scaled, scaled])[None, :]


def attention_kernel(layer, first, x_ref, norm_ref, pos_smem, pos_ref, freq_ref, wq_hbm, wk_hbm, wv_hbm, k_hbm, v_hbm, *rest):
    if not first:
        rest = rest[2:]
    (out_ref, k_out, v_out, wq_buf, wkv_buf, k_buf, v_buf, h_buf, q_buf, kv_buf, mix_buf, w_sem, in_sem, out_sem) = rest
    rows, width = x_ref.shape
    inner = wq_buf.shape[1]
    seq, dim = k_buf.shape[1], k_buf.shape[2]
    heads = inner // dim
    chunk = width // CHUNKS
    groups = rows // GROUP

    def load_weights(i):
        ks = pl.ds(i * chunk, chunk)
        return (pltpu.make_async_copy(wq_hbm.at[layer, ks], wq_buf.at[ks], w_sem.at[0, i]),
                pltpu.make_async_copy(wk_hbm.at[layer, ks], wkv_buf.at[ks, pl.ds(0, dim)], w_sem.at[1, i]),
                pltpu.make_async_copy(wv_hbm.at[layer, ks], wkv_buf.at[ks, pl.ds(dim, dim)], w_sem.at[2, i]))

    load_k = pltpu.make_async_copy(k_hbm.at[layer], k_buf, in_sem.at[0])
    load_v = pltpu.make_async_copy(v_hbm.at[layer], v_buf, in_sem.at[1])
    for i in range(CHUNKS):
        for copy in load_weights(i):
            copy.start()
    load_k.start()
    load_v.start()

    sum_sq = jnp.zeros((rows, 1), jnp.float32)
    for i in range(CHUNKS):
        part = x_ref[:, pl.ds(i * chunk, chunk)].astype(jnp.float32)
        sum_sq = sum_sq + jnp.sum(part * part, axis=-1, keepdims=True)
    scale = lax.rsqrt(sum_sq / width + 1e-5)
    for i in range(CHUNKS):
        cols = pl.ds(i * chunk, chunk)
        h_buf[:, cols] = (x_ref[:, cols].astype(jnp.float32) * scale * norm_ref[layer:layer + 1, cols].astype(jnp.float32)).astype(jnp.bfloat16)

    square = (rows, rows)
    diagonal = lax.broadcasted_iota(jnp.int32, square, 0) == lax.broadcasted_iota(jnp.int32, square, 1)
    column = jnp.sum(jnp.where(diagonal, jnp.broadcast_to(pos_ref[...].astype(jnp.float32), square), 0.0), axis=-1, keepdims=True)
    angles = column * freq_ref[...]
    lane = lax.broadcasted_iota(jnp.int32, (rows, dim), 1)
    cos_tab = jnp.cos(angles)
    sin_tab = jnp.where(lane < dim // 2, -jnp.sin(angles), jnp.sin(angles))

    for i in range(CHUNKS):
        for copy in load_weights(i):
            copy.wait()
        ks = pl.ds(i * chunk, chunk)
        q_part = jnp.dot(h_buf[:, ks], wq_buf[ks, :], preferred_element_type=jnp.float32)
        kv_part = jnp.dot(h_buf[:, ks], wkv_buf[ks, :], preferred_element_type=jnp.float32)
        if i == 0:
            q_buf[...] = q_part
            kv_buf[...] = kv_part
        else:
            q_buf[...] += q_part
            kv_buf[...] += kv_part

    def rounded(value):
        return value.astype(jnp.bfloat16).astype(jnp.float32)

    def rope(vec):
        vec = rounded(vec)
        half = dim // 2
        swapped = jnp.concatenate([vec[:, half:], vec[:, :half]], axis=-1)
        return rounded(vec * cos_tab + swapped * sin_tab)

    for j in range(heads):
        cols = pl.ds(j * dim, dim)
        q_buf[:, cols] = rope(q_buf[:, cols])
    kv_buf[:, pl.ds(0, dim)] = rope(kv_buf[:, pl.ds(0, dim)])
    kv_buf[:, pl.ds(dim, dim)] = rounded(kv_buf[:, pl.ds(dim, dim)])

    load_k.wait()
    load_v.wait()

    def store(g):
        part = pl.ds(pl.multiple_of(g * GROUP, GROUP), GROUP)
        return (pltpu.make_async_copy(k_buf.at[part], k_out.at[layer, part], out_sem.at[0, g]),
                pltpu.make_async_copy(v_buf.at[part], v_out.at[layer, part], out_sem.at[1, g]))

    def update(g, carry):
        base = pl.multiple_of(g * GROUP, GROUP)
        fresh = kv_buf[pl.ds(base, GROUP), :]
        for i in range(GROUP):
            pos = pos_smem[base + i]
            top = pl.multiple_of((pos // ROWS) * ROWS, ROWS)
            here = lax.broadcasted_iota(jnp.int32, (ROWS, dim), 0) == pos - top
            for buf, off in ((k_buf, 0), (v_buf, dim)):
                old = buf[base + i, pl.ds(top, ROWS), :].astype(jnp.float32)
                new = jnp.broadcast_to(fresh[i:i + 1, off:off + dim], (ROWS, dim))
                buf[base + i, pl.ds(top, ROWS), :] = jnp.where(here, new, old).astype(jnp.bfloat16)

        @pl.when(g > 0)
        def _():
            for copy in store(g - 1):
                copy.start()
        return carry

    lax.fori_loop(0, groups, update, 0)
    for copy in store(groups - 1):
        copy.start()

    request = lax.rem(lax.broadcasted_iota(jnp.int32, (heads * GROUP, 1), 0), GROUP)
    first_col = request * seq
    col = lax.broadcasted_iota(jnp.int32, (heads * GROUP, GROUP * seq), 1)

    def attend(step, carry):
        done = []
        for k in range(TOGETHER):
            base = pl.multiple_of((step * TOGETHER + k) * GROUP, GROUP)
            block = pl.ds(base, GROUP)
            last_col = first_col
            for i in range(GROUP):
                last_col = jnp.where(request == i, i * seq + pos_smem[base + i], last_col)
            query = jnp.concatenate([q_buf[block, pl.ds(j * dim, dim)] for j in range(heads)], axis=0).astype(jnp.bfloat16)
            keys = k_buf[block].reshape(GROUP * seq, dim)
            values = v_buf[block].reshape(GROUP * seq, dim)
            scores = lax.dot_general(query, keys, (((1,), (1,)), ((), ())), preferred_element_type=jnp.float32) * (dim ** -0.5)
            scores = jnp.where((col >= first_col) & (col <= last_col), scores, -jnp.inf)
            weight = jnp.exp(scores - jnp.max(scores, axis=-1, keepdims=True))
            prob = (weight * (1.0 / jnp.sum(weight, axis=-1, keepdims=True))).astype(jnp.bfloat16)
            done.append((block, jnp.dot(prob, values, preferred_element_type=jnp.float32)))
        for block, mixed in done:
            for j in range(heads):
                mix_buf[block, pl.ds(j * dim, dim)] = mixed[j * GROUP:(j + 1) * GROUP]
        return carry

    lax.fori_loop(0, groups // TOGETHER, attend, 0)
    out_ref[...] = mix_buf[...].astype(jnp.bfloat16)

    def drain(g, carry):
        for copy in store(g):
            copy.wait()
        return carry

    lax.fori_loop(0, groups, drain, 0)


CHUNKS = 4
GROUP = 8
ROWS = 16
TOGETHER = 4


def attention_call(layer, x, norm, positions, freqs, w_query, w_key, w_value, k_cache, v_cache, k_done, v_done):
    rows, width = x.shape
    inner = w_query.shape[2]
    seq, dim = k_cache.shape[2], k_cache.shape[3]
    bf16 = jnp.bfloat16
    first = k_done is None
    vmem = pl.BlockSpec(memory_space=pltpu.VMEM)
    hbm = pl.BlockSpec(memory_space=pltpu.HBM)
    smem = pl.BlockSpec(memory_space=pltpu.SMEM)
    args = [x, norm, positions, positions[None, :], freqs, w_query, w_key, w_value, k_cache, v_cache]
    specs = [vmem, vmem, smem, vmem, vmem, hbm, hbm, hbm, hbm, hbm]
    aliases = {}
    if not first:
        aliases = {len(args): 1, len(args) + 1: 2}
        args += [k_done, v_done]
        specs += [hbm, hbm]
    weights = width * (inner + 2 * dim)
    return pl.pallas_call(
        functools.partial(attention_kernel, layer, first),
        out_shape=[jax.ShapeDtypeStruct((rows, inner), bf16), jax.ShapeDtypeStruct(k_cache.shape, bf16), jax.ShapeDtypeStruct(v_cache.shape, bf16)],
        in_specs=specs,
        out_specs=[vmem, hbm, hbm],
        scratch_shapes=[
            pltpu.VMEM((width, inner), bf16),
            pltpu.VMEM((width, 2 * dim), bf16),
            pltpu.VMEM((rows, seq, dim), bf16),
            pltpu.VMEM((rows, seq, dim), bf16),
            pltpu.VMEM((rows, width), bf16),
            pltpu.VMEM((rows, inner), jnp.float32),
            pltpu.VMEM((rows, 2 * dim), jnp.float32),
            pltpu.VMEM((rows, inner), jnp.float32),
            pltpu.SemaphoreType.DMA((3, CHUNKS)),
            pltpu.SemaphoreType.DMA((2,)),
            pltpu.SemaphoreType.DMA((2, rows // GROUP)),
        ],
        input_output_aliases=aliases,
        compiler_params=pltpu.CompilerParams(vmem_limit_bytes=67043328),
        cost_estimate=pl.CostEstimate(flops=2 * rows * weights, bytes_accessed=2 * weights, transcendentals=rows * seq),
        name='attention_layer',
    )(*args)


PIECES = 5
TILE = 256


def mlp_kernel(layer, chips, attn_ref, res_ref, norm_ref, wo_hbm, wg_hbm, wu_hbm, wd_hbm, out_ref,
               o_buf, g_buf, u_buf, d_buf, full, part, act, res, swap_in, summed, owner_in,
               w_sem, io_sem, rs_send, rs_recv, ag_send, ag_recv):
    rows, width = full.shape
    piece = width // PIECES
    half_rows = rows // 2
    own_rows = half_rows // chips
    me = lax.axis_index('tp')
    core = lax.rem(me, 2)
    chip = me // 2
    partner = me + 1 - 2 * core
    peers = [2 * lax.rem(chip + hop, chips) + core for hop in range(chips)]
    hops = tuple(sorted(range(1, chips), key=lambda hop: -min(hop, chips - hop)))
    nearest = hops[::-1]
    n_gate = g_buf.shape[0]

    def piece_cols(p):
        return pl.ds(p * piece, piece)

    def rows_of(offset):
        return pl.ds(pl.multiple_of(core * half_rows + lax.rem(chip + offset, chips) * own_rows, own_rows), own_rows)

    def block(offset):
        return pl.ds(pl.multiple_of(lax.rem(chip + offset, chips) * own_rows, own_rows), own_rows)

    mine = rows_of(0)
    other_rows = pl.ds(pl.multiple_of((1 - core) * half_rows, half_rows), half_rows)
    my_rows = pl.ds(pl.multiple_of(core * half_rows, half_rows), half_rows)

    def load_out(p):
        return pltpu.make_async_copy(wo_hbm.at[layer, :, piece_cols(p)], o_buf.at[p], w_sem.at[p])

    def load_down(p):
        return pltpu.make_async_copy(wd_hbm.at[layer, :, piece_cols(p)], d_buf.at[p], w_sem.at[PIECES + p])

    def load_gate(j):
        cols = pl.ds(pl.multiple_of(j * TILE, TILE), TILE)
        return pltpu.make_async_copy(wg_hbm.at[layer, :, cols], g_buf.at[j], w_sem.at[2 * PIECES + j])

    def load_up(j):
        cols = pl.ds(pl.multiple_of(j * TILE, TILE), TILE)
        return pltpu.make_async_copy(wu_hbm.at[layer, :, cols], u_buf.at[j], w_sem.at[2 * PIECES + n_gate + j])

    load_res = pltpu.make_async_copy(res_ref.at[mine], res, io_sem.at[0])

    def store(p):
        return pltpu.make_async_copy(full.at[:, piece_cols(p)], out_ref.at[:, piece_cols(p)], io_sem.at[1 + p])

    for p in range(PIECES):
        load_out(p).start()
    load_res.start()

    def start_gate_up():
        for j in range(n_gate):
            load_gate(j).start()
            load_up(j).start()

    def start_down():
        for p in range(PIECES):
            load_down(p).start()

    barrier = pltpu.get_barrier_semaphore()
    for peer in [partner] + peers[1:]:
        pl.semaphore_signal(barrier, inc=1, device_id={'tp': peer}, device_id_type=pl.DeviceIdType.MESH)
    pl.semaphore_wait(barrier, chips)

    def remote(src, dst, send_sem, recv_sem, peer):
        return pltpu.make_async_remote_copy(src_ref=src, dst_ref=dst, send_sem=send_sem, recv_sem=recv_sem, device_id={'tp': peer}, device_id_type=pl.DeviceIdType.MESH)

    def swap(p):
        return remote(part.at[other_rows, piece_cols(p)], swap_in.at[p], rs_send.at[0, p], rs_recv.at[0, p], partner)

    def to_owner(p, hop):
        return remote(summed.at[p, block(hop)], owner_in.at[hop - 1, p], rs_send.at[hop, p], rs_recv.at[hop, p], peers[hop])

    def spread(p, hop):
        return remote(res.at[:, piece_cols(p)], full.at[mine, piece_cols(p)], ag_send.at[hop, p], ag_recv.at[hop, p], peers[hop] if hop else partner)

    def forward(p, hop):
        landed = full.at[rows_of(chips - hop), piece_cols(p)]
        return remote(landed, landed, ag_send.at[chips + hop - 1, p], ag_recv.at[chips + hop - 1, p], partner)

    def add_over_tp(lhs_ref, w_buf, load, after_products, after_sums):
        def product(p):
            load(p).wait()
            for i in range(piece // TILE):
                part[:, pl.ds(p * piece + i * TILE, TILE)] = jnp.dot(
                    lhs_ref[...], w_buf[p, :, pl.ds(i * TILE, TILE)], preferred_element_type=jnp.float32).astype(jnp.bfloat16)
            swap(p).start()

        def chip_sum(p):
            swap(p).wait_recv()
            summed[p] = (part[my_rows, piece_cols(p)].astype(jnp.float32) + swap_in[p].astype(jnp.float32)).astype(jnp.bfloat16)
            for hop in hops:
                to_owner(p, hop).start()

        product(0)
        for p in range(1, PIECES):
            product(p)
            chip_sum(p - 1)
        after_products()
        chip_sum(PIECES - 1)
        after_sums()
        for p in range(PIECES):
            total = summed[p, block(0)].astype(jnp.float32)
            for hop in range(1, chips):
                to_owner(p, hop).wait_recv()
                total = total + owner_in[hop - 1, p].astype(jnp.float32)
            new = res[:, piece_cols(p)].astype(jnp.float32) + total.astype(jnp.bfloat16).astype(jnp.float32)
            new = new.astype(jnp.bfloat16)
            res[:, piece_cols(p)] = new
            full[mine, piece_cols(p)] = new
            for hop in hops + (0,):
                spread(p, hop).start()
        for p in range(PIECES):
            for hop in nearest:
                spread(p, hop).wait_recv()
                forward(p, hop).start()

    def gathered(p):
        spread(p, 0).wait_recv()
        for hop in nearest:
            forward(p, hop).wait_recv()

    def drain_sends():
        for p in range(PIECES):
            swap(p).wait_send()
            for hop in range(1, chips):
                to_owner(p, hop).wait_send()
                forward(p, hop).wait_send()
            for hop in range(chips):
                spread(p, hop).wait_send()

    load_res.wait()
    add_over_tp(attn_ref, o_buf, load_out, start_gate_up, start_down)
    sum_sq = jnp.zeros((rows, 1), jnp.float32)
    for p in range(PIECES):
        gathered(p)
        new = full[:, piece_cols(p)].astype(jnp.float32)
        sum_sq = sum_sq + jnp.sum(new * new, axis=-1, keepdims=True)
    drain_sends()
    scale = lax.rsqrt(sum_sq / width + 1e-5)
    for p in range(PIECES):
        cols = piece_cols(p)
        part[:, cols] = (full[:, cols].astype(jnp.float32) * scale * norm_ref[layer:layer + 1, cols].astype(jnp.float32)).astype(jnp.bfloat16)

    def gate_up(j, carry):
        load_gate(j).wait()
        load_up(j).wait()
        gate = jnp.dot(part[...], g_buf[j], preferred_element_type=jnp.float32).astype(jnp.bfloat16).astype(jnp.float32)
        up = jnp.dot(part[...], u_buf[j], preferred_element_type=jnp.float32).astype(jnp.bfloat16).astype(jnp.float32)
        act[:, pl.ds(pl.multiple_of(j * TILE, TILE), TILE)] = (gate * jax.nn.sigmoid(gate) * up).astype(jnp.bfloat16)
        return carry

    lax.fori_loop(0, n_gate, gate_up, 0)
    add_over_tp(act, d_buf, load_down, lambda: None, lambda: None)
    for p in range(PIECES):
        gathered(p)
        store(p).start()
    drain_sends()
    for p in range(PIECES):
        store(p).wait()


def mlp_call(layer, chips, attended, hidden, norm, w_out, w_gate, w_up, w_down):
    rows, inner = attended.shape
    width = w_gate.shape[1]
    ff = w_gate.shape[2]
    piece = width // PIECES
    own_rows = rows // 2 // chips
    bf16 = jnp.bfloat16
    vmem = pl.BlockSpec(memory_space=pltpu.VMEM)
    hbm = pl.BlockSpec(memory_space=pltpu.HBM)
    scratch = [
        pltpu.VMEM((PIECES, inner, piece), bf16),
        pltpu.VMEM((ff // TILE, width, TILE), bf16),
        pltpu.VMEM((ff // TILE, width, TILE), bf16),
        pltpu.VMEM((PIECES, ff, piece), bf16),
        pltpu.VMEM((rows, width), bf16),
        pltpu.VMEM((rows, width), bf16),
        pltpu.VMEM((rows, ff), bf16),
        pltpu.VMEM((own_rows, width), bf16),
        pltpu.VMEM((PIECES, rows // 2, piece), bf16),
        pltpu.VMEM((PIECES, rows // 2, piece), bf16),
        pltpu.VMEM((chips - 1, PIECES, own_rows, piece), bf16),
        pltpu.SemaphoreType.DMA((2 * PIECES + 2 * (ff // TILE),)),
        pltpu.SemaphoreType.DMA((1 + PIECES,)),
        pltpu.SemaphoreType.DMA((chips, PIECES)),
        pltpu.SemaphoreType.DMA((chips, PIECES)),
        pltpu.SemaphoreType.DMA((2 * chips - 1, PIECES)),
        pltpu.SemaphoreType.DMA((2 * chips - 1, PIECES)),
    ]
    weights = inner * width + 3 * width * ff
    return pl.pallas_call(
        functools.partial(mlp_kernel, layer, chips),
        out_shape=jax.ShapeDtypeStruct((rows, width), bf16),
        in_specs=[vmem, hbm, vmem, hbm, hbm, hbm, hbm],
        out_specs=hbm,
        scratch_shapes=scratch,
        compiler_params=pltpu.CompilerParams(collective_id=layer, has_side_effects=True, vmem_limit_bytes=67043328),
        cost_estimate=pl.CostEstimate(flops=2 * rows * weights, bytes_accessed=2 * weights, transcendentals=rows * ff),
        name='mlp_layer',
    )(attended, hidden, norm, w_out, w_gate, w_up, w_down)


def solution(mesh):
    row_spec = P('dp', None)
    pos_spec = P('dp')
    cache_spec = P(None, 'dp', None, 'tp', None)
    norm_spec = P(None, None)
    col_spec = P(None, None, 'tp')
    split_rows = P(None, 'tp', None)
    chips = mesh.shape['tp'] // 2

    def local_step(hidden, positions, k_cache, v_cache, attn_norm, w_query, w_key, w_value, w_out, mlp_norm, w_gate, w_up, w_down):
        layers, batch, seq, kv_heads, dim = k_cache.shape
        freqs = rope_freqs(dim)
        k_old = k_cache.reshape(layers, batch, seq, dim)
        v_old = v_cache.reshape(layers, batch, seq, dim)
        k_out = v_out = None
        for layer in range(layers):
            attended, k_out, v_out = attention_call(layer, hidden, attn_norm, positions, freqs, w_query, w_key, w_value, k_old, v_old, k_out, v_out)
            hidden = mlp_call(layer, chips, attended, hidden, mlp_norm, w_out, w_gate, w_up, w_down)
        shape = (layers, batch, seq, kv_heads, dim)
        return hidden, k_out.reshape(shape), v_out.reshape(shape)

    return jax.shard_map(local_step, mesh=mesh, in_specs=(row_spec, pos_spec, cache_spec, cache_spec, norm_spec, col_spec, col_spec, col_spec, split_rows, norm_spec, col_spec, col_spec, split_rows), out_specs=(row_spec, cache_spec, cache_spec), check_vma=False)
```

```python
import functools
import math
import jax
import jax.numpy as jnp
import numpy as np
from jax import lax
from jax.experimental import pallas as pl
from jax.experimental.pallas import tpu as pltpu
from jax.sharding import PartitionSpec as P


def rope_freqs(head_dim):
    half_dim = head_dim // 2
    inv_freq = np.power(np.float64(500000.0), -np.arange(half_dim) * (2.0 / head_dim))
    wavelen = (2.0 * math.pi) / inv_freq
    smooth = (8192.0 / wavelen - 1.0) / 3.0
    blended = (1.0 - smooth) * inv_freq / 8.0 + smooth * inv_freq
    scaled = np.where(wavelen < 2048.0, inv_freq, np.where(wavelen > 8192.0, inv_freq / 8.0, blended))
    return np.concatenate([scaled, scaled])[None, :].astype(np.float32)


def attention_kernel(layer, first, x_ref, norm_ref, pos_smem, pos_ref, freq_ref, wq_hbm, wk_hbm, wv_hbm, k_hbm, v_hbm, *rest):
    if not first:
        rest = rest[2:]
    (out_ref, k_out, v_out, wq_buf, wkv_buf, k_buf, v_buf, h_buf, q_buf, kv_buf, mix_buf, prob_buf, att_buf, x_buf, norm_buf, w_sem, in_sem, out_sem) = rest
    rows, width = x_ref.shape
    inner = wq_buf.shape[1]
    seq, dim = k_buf.shape[1], k_buf.shape[2]
    heads = inner // dim
    chunk = width // CHUNKS
    groups = rows // GROUP

    def load_weights(i):
        ks = pl.ds(i * chunk, chunk)
        return (pltpu.make_async_copy(wq_hbm.at[layer, ks], wq_buf.at[ks], w_sem.at[0, i]),
                pltpu.make_async_copy(wk_hbm.at[layer, ks], wkv_buf.at[ks, pl.ds(0, dim)], w_sem.at[1, i]),
                pltpu.make_async_copy(wv_hbm.at[layer, ks], wkv_buf.at[ks, pl.ds(dim, dim)], w_sem.at[2, i]))

    load_k = pltpu.make_async_copy(k_hbm.at[layer], k_buf, in_sem.at[0])
    load_v = pltpu.make_async_copy(v_hbm.at[layer], v_buf, in_sem.at[1])
    load_x = pltpu.make_async_copy(x_ref, x_buf, in_sem.at[3])
    load_norm = pltpu.make_async_copy(norm_ref, norm_buf, in_sem.at[4])
    load_x.start()
    load_norm.start()
    for i in range(CHUNKS):
        for copy in load_weights(i):
            copy.start()
    load_k.start()
    load_v.start()

    load_x.wait()
    load_norm.wait()
    sum_sq = jnp.zeros((rows, 1), jnp.float32)
    for i in range(CHUNKS):
        part = x_buf[:, pl.ds(i * chunk, chunk)].astype(jnp.float32)
        sum_sq = sum_sq + jnp.sum(part * part, axis=-1, keepdims=True)
    scale = lax.rsqrt(sum_sq / width + 1e-5)
    for i in range(CHUNKS):
        cols = pl.ds(i * chunk, chunk)
        h_buf[:, cols] = (x_buf[:, cols].astype(jnp.float32) * scale * norm_buf[layer:layer + 1, cols].astype(jnp.float32)).astype(jnp.bfloat16)

    square = (rows, rows)
    diagonal = lax.broadcasted_iota(jnp.int32, square, 0) == lax.broadcasted_iota(jnp.int32, square, 1)
    column = jnp.sum(jnp.where(diagonal, jnp.broadcast_to(pos_ref[...].astype(jnp.float32), square), 0.0), axis=-1, keepdims=True)
    angles = column * freq_ref[...]
    lane = lax.broadcasted_iota(jnp.int32, (rows, dim), 1)
    cos_tab = jnp.cos(angles)
    sin_tab = jnp.where(lane < dim // 2, -jnp.sin(angles), jnp.sin(angles))

    for i in range(CHUNKS):
        for copy in load_weights(i):
            copy.wait()
        ks = pl.ds(i * chunk, chunk)
        q_part = jnp.dot(h_buf[:, ks], wq_buf[ks, :], preferred_element_type=jnp.float32)
        kv_part = jnp.dot(h_buf[:, ks], wkv_buf[ks, :], preferred_element_type=jnp.float32)
        if i == 0:
            q_buf[...] = q_part
            kv_buf[...] = kv_part
        else:
            q_buf[...] += q_part
            kv_buf[...] += kv_part

    def rounded(value):
        return value.astype(jnp.bfloat16).astype(jnp.float32)

    def rope(vec):
        vec = rounded(vec)
        half = dim // 2
        swapped = jnp.concatenate([vec[:, half:], vec[:, :half]], axis=-1)
        return rounded(vec * cos_tab + swapped * sin_tab)

    for j in range(heads):
        cols = pl.ds(j * dim, dim)
        q_buf[:, cols] = rope(q_buf[:, cols])
    kv_buf[:, pl.ds(0, dim)] = rope(kv_buf[:, pl.ds(0, dim)])
    kv_buf[:, pl.ds(dim, dim)] = rounded(kv_buf[:, pl.ds(dim, dim)])

    load_k.wait()
    load_v.wait()

    def store(g):
        part = pl.ds(pl.multiple_of(g * GROUP, GROUP), GROUP)
        return (pltpu.make_async_copy(k_buf.at[part], k_out.at[layer, part], out_sem.at[0, g]),
                pltpu.make_async_copy(v_buf.at[part], v_out.at[layer, part], out_sem.at[1, g]))

    def update(g, carry):
        base = pl.multiple_of(g * GROUP, GROUP)
        fresh = kv_buf[pl.ds(base, GROUP), :]
        for i in range(GROUP):
            pos = pos_smem[base + i]
            top = pl.multiple_of((pos // ROWS) * ROWS, ROWS)
            here = lax.broadcasted_iota(jnp.int32, (ROWS, dim), 0) == pos - top
            for buf, off in ((k_buf, 0), (v_buf, dim)):
                old = buf[base + i, pl.ds(top, ROWS), :].astype(jnp.float32)
                new = jnp.broadcast_to(fresh[i:i + 1, off:off + dim], (ROWS, dim))
                buf[base + i, pl.ds(top, ROWS), :] = jnp.where(here, new, old).astype(jnp.bfloat16)

        @pl.when(g > 0)
        def _():
            for copy in store(g - 1):
                copy.start()
        return carry

    lax.fori_loop(0, groups, update, 0)
    for copy in store(groups - 1):
        copy.start()

    request = lax.rem(lax.broadcasted_iota(jnp.int32, (heads * GROUP, 1), 0), GROUP)
    first_col = request * seq
    col = lax.broadcasted_iota(jnp.int32, (heads * GROUP, GROUP * seq), 1)

    def weigh(step, carry):
        done = []
        for k in range(TOGETHER):
            g = step * TOGETHER + k
            base = pl.multiple_of(g * GROUP, GROUP)
            block = pl.ds(base, GROUP)
            last_col = first_col
            for i in range(GROUP):
                last_col = jnp.where(request == i, i * seq + pos_smem[base + i], last_col)
            query = jnp.concatenate([q_buf[block, pl.ds(j * dim, dim)] for j in range(heads)], axis=0).astype(jnp.bfloat16)
            keys = k_buf[block].reshape(GROUP * seq, dim)
            scores = lax.dot_general(query, keys, (((1,), (1,)), ((), ())), preferred_element_type=jnp.float32) * (dim ** -0.5)
            scores = jnp.where((col >= first_col) & (col <= last_col), scores, -jnp.inf)
            weight = jnp.exp(scores - jnp.max(scores, axis=-1, keepdims=True))
            done.append((g, (weight * (1.0 / jnp.sum(weight, axis=-1, keepdims=True))).astype(jnp.bfloat16)))
        for g, prob in done:
            prob_buf[g] = prob
        return carry

    def mix(step, carry):
        done = []
        for k in range(TOGETHER):
            g = step * TOGETHER + k
            block = pl.ds(pl.multiple_of(g * GROUP, GROUP), GROUP)
            values = v_buf[block].reshape(GROUP * seq, dim)
            done.append((block, jnp.dot(prob_buf[g], values, preferred_element_type=jnp.float32)))
        for block, mixed in done:
            for j in range(heads):
                mix_buf[block, pl.ds(j * dim, dim)] = mixed[j * GROUP:(j + 1) * GROUP]
        return carry

    lax.fori_loop(0, groups // TOGETHER, weigh, 0)
    lax.fori_loop(0, groups // TOGETHER, mix, 0)
    att_buf[...] = mix_buf[...].astype(jnp.bfloat16)
    store_out = pltpu.make_async_copy(att_buf, out_ref, in_sem.at[2])
    store_out.start()

    def drain(g, carry):
        for copy in store(g):
            copy.wait()
        return carry

    lax.fori_loop(0, groups, drain, 0)
    store_out.wait()


CHUNKS = 4
GROUP = 8
ROWS = 16
TOGETHER = 4


def attention_call(layer, x, norm, positions, freqs, w_query, w_key, w_value, k_cache, v_cache, k_done, v_done):
    rows, width = x.shape
    inner = w_query.shape[2]
    seq, dim = k_cache.shape[2], k_cache.shape[3]
    bf16 = jnp.bfloat16
    first = k_done is None
    vmem = pl.BlockSpec(memory_space=pltpu.VMEM)
    hbm = pl.BlockSpec(memory_space=pltpu.HBM)
    smem = pl.BlockSpec(memory_space=pltpu.SMEM)
    args = [x, norm, positions, positions[None, :], freqs, w_query, w_key, w_value, k_cache, v_cache]
    specs = [hbm, hbm, smem, vmem, vmem, hbm, hbm, hbm, hbm, hbm]
    aliases = {}
    if not first:
        aliases = {len(args): 1, len(args) + 1: 2}
        args += [k_done, v_done]
        specs += [hbm, hbm]
    weights = width * (inner + 2 * dim)
    return pl.pallas_call(
        functools.partial(attention_kernel, layer, first),
        out_shape=[jax.ShapeDtypeStruct((rows, inner), bf16), jax.ShapeDtypeStruct(k_cache.shape, bf16), jax.ShapeDtypeStruct(v_cache.shape, bf16)],
        in_specs=specs,
        out_specs=[hbm, hbm, hbm],
        scratch_shapes=[
            pltpu.VMEM((width, inner), bf16),
            pltpu.VMEM((width, 2 * dim), bf16),
            pltpu.VMEM((rows, seq, dim), bf16),
            pltpu.VMEM((rows, seq, dim), bf16),
            pltpu.VMEM((rows, width), bf16),
            pltpu.VMEM((rows, inner), jnp.float32),
            pltpu.VMEM((rows, 2 * dim), jnp.float32),
            pltpu.VMEM((rows, inner), jnp.float32),
            pltpu.VMEM((rows // GROUP, GROUP * inner // dim, GROUP * seq), bf16),
            pltpu.VMEM((rows, inner), bf16),
            pltpu.VMEM((rows, width), bf16),
            pltpu.VMEM(norm.shape, bf16),
            pltpu.SemaphoreType.DMA((3, CHUNKS)),
            pltpu.SemaphoreType.DMA((5,)),
            pltpu.SemaphoreType.DMA((2, rows // GROUP)),
        ],
        input_output_aliases=aliases,
        compiler_params=pltpu.CompilerParams(vmem_limit_bytes=67043328),
        cost_estimate=pl.CostEstimate(flops=2 * rows * weights, bytes_accessed=2 * weights, transcendentals=rows * seq),
        name='attention_layer',
    )(*args)


PIECES = 5
TILE = 256


def mlp_kernel(layer, chips, attn_hbm, res_ref, norm_hbm, wo_hbm, wg_hbm, wu_hbm, wd_hbm, out_ref,
               o_buf, g_buf, u_buf, d_buf, full, part, act, res, attn_ref, norm_ref, swap_in, summed, owner_in,
               w_sem, io_sem, rs_send, rs_recv, ag_send, ag_recv):
    rows, width = full.shape
    piece = width // PIECES
    half_rows = rows // 2
    own_rows = half_rows // chips
    me = lax.axis_index('tp')
    core = lax.rem(me, 2)
    chip = me // 2
    partner = me + 1 - 2 * core
    peers = [2 * lax.rem(chip + hop, chips) + core for hop in range(chips)]
    hops = tuple(sorted(range(1, chips), key=lambda hop: -min(hop, chips - hop)))
    nearest = hops[::-1]
    n_gate = g_buf.shape[0]

    def piece_cols(p):
        return pl.ds(p * piece, piece)

    def rows_of(offset):
        return pl.ds(pl.multiple_of(core * half_rows + lax.rem(chip + offset, chips) * own_rows, own_rows), own_rows)

    def block(offset):
        return pl.ds(pl.multiple_of(lax.rem(chip + offset, chips) * own_rows, own_rows), own_rows)

    mine = rows_of(0)
    other_rows = pl.ds(pl.multiple_of((1 - core) * half_rows, half_rows), half_rows)
    my_rows = pl.ds(pl.multiple_of(core * half_rows, half_rows), half_rows)

    def load_out(p):
        return pltpu.make_async_copy(wo_hbm.at[layer, :, piece_cols(p)], o_buf.at[p], w_sem.at[p])

    def load_down(p):
        return pltpu.make_async_copy(wd_hbm.at[layer, :, piece_cols(p)], d_buf.at[p], w_sem.at[PIECES + p])

    def load_gate(j):
        cols = pl.ds(pl.multiple_of(j * TILE, TILE), TILE)
        return pltpu.make_async_copy(wg_hbm.at[layer, :, cols], g_buf.at[j], w_sem.at[2 * PIECES + j])

    def load_up(j):
        cols = pl.ds(pl.multiple_of(j * TILE, TILE), TILE)
        return pltpu.make_async_copy(wu_hbm.at[layer, :, cols], u_buf.at[j], w_sem.at[2 * PIECES + n_gate + j])

    load_res = pltpu.make_async_copy(res_ref.at[mine], res, io_sem.at[0])
    load_attn = pltpu.make_async_copy(attn_hbm, attn_ref, io_sem.at[1 + PIECES])
    load_norm = pltpu.make_async_copy(norm_hbm, norm_ref, io_sem.at[2 + PIECES])

    def store(p):
        return pltpu.make_async_copy(full.at[:, piece_cols(p)], out_ref.at[:, piece_cols(p)], io_sem.at[1 + p])

    load_attn.start()
    for p in range(PIECES):
        load_out(p).start()
    load_res.start()
    load_norm.start()

    def start_gate_up():
        for j in range(n_gate):
            load_gate(j).start()
            load_up(j).start()

    def start_down():
        for p in range(PIECES):
            load_down(p).start()

    barrier = pltpu.get_barrier_semaphore()
    for peer in [partner] + peers[1:]:
        pl.semaphore_signal(barrier, inc=1, device_id={'tp': peer}, device_id_type=pl.DeviceIdType.MESH)
    pl.semaphore_wait(barrier, chips)

    def remote(src, dst, send_sem, recv_sem, peer):
        return pltpu.make_async_remote_copy(src_ref=src, dst_ref=dst, send_sem=send_sem, recv_sem=recv_sem, device_id={'tp': peer}, device_id_type=pl.DeviceIdType.MESH)

    def swap(p):
        return remote(part.at[other_rows, piece_cols(p)], swap_in.at[p], rs_send.at[0, p], rs_recv.at[0, p], partner)

    def to_owner(p, hop):
        return remote(summed.at[p, block(hop)], owner_in.at[hop - 1, p], rs_send.at[hop, p], rs_recv.at[hop, p], peers[hop])

    def spread(p, hop):
        return remote(res.at[:, piece_cols(p)], full.at[mine, piece_cols(p)], ag_send.at[hop, p], ag_recv.at[hop, p], peers[hop] if hop else partner)

    def forward(p, hop):
        landed = full.at[rows_of(chips - hop), piece_cols(p)]
        return remote(landed, landed, ag_send.at[chips + hop - 1, p], ag_recv.at[chips + hop - 1, p], partner)

    def add_over_tp(lhs_ref, w_buf, load, after_products, after_sums):
        def product(p):
            load(p).wait()
            for i in range(piece // TILE):
                part[:, pl.ds(p * piece + i * TILE, TILE)] = jnp.dot(
                    lhs_ref[...], w_buf[p, :, pl.ds(i * TILE, TILE)], preferred_element_type=jnp.float32).astype(jnp.bfloat16)
            swap(p).start()

        def chip_sum(p):
            swap(p).wait_recv()
            summed[p] = (part[my_rows, piece_cols(p)].astype(jnp.float32) + swap_in[p].astype(jnp.float32)).astype(jnp.bfloat16)
            for hop in hops:
                to_owner(p, hop).start()

        product(0)
        for p in range(1, PIECES):
            product(p)
            chip_sum(p - 1)
        after_products()
        chip_sum(PIECES - 1)
        after_sums()
        for p in range(PIECES):
            total = summed[p, block(0)].astype(jnp.float32)
            for hop in range(1, chips):
                to_owner(p, hop).wait_recv()
                total = total + owner_in[hop - 1, p].astype(jnp.float32)
            new = res[:, piece_cols(p)].astype(jnp.float32) + total.astype(jnp.bfloat16).astype(jnp.float32)
            new = new.astype(jnp.bfloat16)
            res[:, piece_cols(p)] = new
            full[mine, piece_cols(p)] = new
            for hop in hops + (0,):
                spread(p, hop).start()
        for p in range(PIECES):
            for hop in nearest:
                spread(p, hop).wait_recv()
                forward(p, hop).start()

    def gathered(p):
        spread(p, 0).wait_recv()
        for hop in nearest:
            forward(p, hop).wait_recv()

    def drain_sends():
        for p in range(PIECES):
            swap(p).wait_send()
            for hop in range(1, chips):
                to_owner(p, hop).wait_send()
                forward(p, hop).wait_send()
            for hop in range(chips):
                spread(p, hop).wait_send()

    load_attn.wait()
    load_res.wait()
    load_norm.wait()
    add_over_tp(attn_ref, o_buf, load_out, start_gate_up, start_down)
    sum_sq = jnp.zeros((rows, 1), jnp.float32)
    for p in range(PIECES):
        gathered(p)
        new = full[:, piece_cols(p)].astype(jnp.float32)
        sum_sq = sum_sq + jnp.sum(new * new, axis=-1, keepdims=True)
    drain_sends()
    scale = lax.rsqrt(sum_sq / width + 1e-5)
    for p in range(PIECES):
        cols = piece_cols(p)
        part[:, cols] = (full[:, cols].astype(jnp.float32) * scale * norm_ref[layer:layer + 1, cols].astype(jnp.float32)).astype(jnp.bfloat16)

    def gate_up(j, carry):
        load_gate(j).wait()
        load_up(j).wait()
        gate = jnp.dot(part[...], g_buf[j], preferred_element_type=jnp.float32).astype(jnp.bfloat16).astype(jnp.float32)
        up = jnp.dot(part[...], u_buf[j], preferred_element_type=jnp.float32).astype(jnp.bfloat16).astype(jnp.float32)
        act[:, pl.ds(pl.multiple_of(j * TILE, TILE), TILE)] = (gate * jax.nn.sigmoid(gate) * up).astype(jnp.bfloat16)
        return carry

    lax.fori_loop(0, n_gate, gate_up, 0)
    add_over_tp(act, d_buf, load_down, lambda: None, lambda: None)
    for p in range(PIECES):
        gathered(p)
        store(p).start()
    drain_sends()
    for p in range(PIECES):
        store(p).wait()


def mlp_call(layer, chips, attended, hidden, norm, w_out, w_gate, w_up, w_down):
    rows, inner = attended.shape
    width = w_gate.shape[1]
    ff = w_gate.shape[2]
    piece = width // PIECES
    own_rows = rows // 2 // chips
    bf16 = jnp.bfloat16
    hbm = pl.BlockSpec(memory_space=pltpu.HBM)
    scratch = [
        pltpu.VMEM((PIECES, inner, piece), bf16),
        pltpu.VMEM((ff // TILE, width, TILE), bf16),
        pltpu.VMEM((ff // TILE, width, TILE), bf16),
        pltpu.VMEM((PIECES, ff, piece), bf16),
        pltpu.VMEM((rows, width), bf16),
        pltpu.VMEM((rows, width), bf16),
        pltpu.VMEM((rows, ff), bf16),
        pltpu.VMEM((own_rows, width), bf16),
        pltpu.VMEM((rows, inner), bf16),
        pltpu.VMEM(norm.shape, bf16),
        pltpu.VMEM((PIECES, rows // 2, piece), bf16),
        pltpu.VMEM((PIECES, rows // 2, piece), bf16),
        pltpu.VMEM((chips - 1, PIECES, own_rows, piece), bf16),
        pltpu.SemaphoreType.DMA((2 * PIECES + 2 * (ff // TILE),)),
        pltpu.SemaphoreType.DMA((3 + PIECES,)),
        pltpu.SemaphoreType.DMA((chips, PIECES)),
        pltpu.SemaphoreType.DMA((chips, PIECES)),
        pltpu.SemaphoreType.DMA((2 * chips - 1, PIECES)),
        pltpu.SemaphoreType.DMA((2 * chips - 1, PIECES)),
    ]
    weights = inner * width + 3 * width * ff
    return pl.pallas_call(
        functools.partial(mlp_kernel, layer, chips),
        out_shape=jax.ShapeDtypeStruct((rows, width), bf16),
        in_specs=[hbm] * 7,
        out_specs=hbm,
        scratch_shapes=scratch,
        compiler_params=pltpu.CompilerParams(collective_id=layer, has_side_effects=True, vmem_limit_bytes=67043328),
        cost_estimate=pl.CostEstimate(flops=2 * rows * weights, bytes_accessed=2 * weights, transcendentals=rows * ff),
        name='mlp_layer',
    )(attended, hidden, norm, w_out, w_gate, w_up, w_down)


def solution(mesh):
    row_spec = P('dp', None)
    pos_spec = P('dp')
    cache_spec = P(None, 'dp', None, 'tp', None)
    norm_spec = P(None, None)
    col_spec = P(None, None, 'tp')
    split_rows = P(None, 'tp', None)
    chips = mesh.shape['tp'] // 2

    def local_step(hidden, positions, k_cache, v_cache, attn_norm, w_query, w_key, w_value, w_out, mlp_norm, w_gate, w_up, w_down):
        layers, batch, seq, kv_heads, dim = k_cache.shape
        freqs = rope_freqs(dim)
        k_old = k_cache.reshape(layers, batch, seq, dim)
        v_old = v_cache.reshape(layers, batch, seq, dim)
        k_out = v_out = None
        for layer in range(layers):
            attended, k_out, v_out = attention_call(layer, hidden, attn_norm, positions, freqs, w_query, w_key, w_value, k_old, v_old, k_out, v_out)
            hidden = mlp_call(layer, chips, attended, hidden, mlp_norm, w_out, w_gate, w_up, w_down)
        shape = (layers, batch, seq, kv_heads, dim)
        return hidden, k_out.reshape(shape), v_out.reshape(shape)

    return jax.shard_map(local_step, mesh=mesh, in_specs=(row_spec, pos_spec, cache_spec, cache_spec, norm_spec, col_spec, col_spec, col_spec, split_rows, norm_spec, col_spec, col_spec, split_rows), out_specs=(row_spec, cache_spec, cache_spec), check_vma=False)
```

```python
import functools
import math
import jax
import jax.numpy as jnp
import numpy as np
from jax import lax
from jax.experimental import pallas as pl
from jax.experimental.pallas import tpu as pltpu
from jax.sharding import PartitionSpec as P


def rope_freqs(head_dim):
    half_dim = head_dim // 2
    inv_freq = np.power(np.float64(500000.0), -np.arange(half_dim) * (2.0 / head_dim))
    wavelen = (2.0 * math.pi) / inv_freq
    smooth = (8192.0 / wavelen - 1.0) / 3.0
    blended = (1.0 - smooth) * inv_freq / 8.0 + smooth * inv_freq
    scaled = np.where(wavelen < 2048.0, inv_freq, np.where(wavelen > 8192.0, inv_freq / 8.0, blended))
    return np.concatenate([scaled, scaled])[None, :].astype(np.float32)


def attention_kernel(layer, first, x_ref, norm_ref, pos_smem, pos_ref, freq_ref, wq_hbm, wk_hbm, wv_hbm, k_hbm, v_hbm, *rest):
    if not first:
        rest = rest[2:]
    (out_ref, k_out, v_out, wq_buf, wkv_buf, k_buf, v_buf, h_buf, q_buf, kv_buf, mix_buf, prob_buf, att_buf, x_buf, norm_buf, w_sem, in_sem, out_sem) = rest
    rows, width = x_ref.shape
    inner = wq_buf.shape[1]
    seq, dim = k_buf.shape[1], k_buf.shape[2]
    heads = inner // dim
    chunk = width // CHUNKS
    groups = rows // GROUP

    def load_weights(i):
        ks = pl.ds(i * chunk, chunk)
        return (pltpu.make_async_copy(wq_hbm.at[layer, ks], wq_buf.at[ks], w_sem.at[0, i]),
                pltpu.make_async_copy(wk_hbm.at[layer, ks], wkv_buf.at[ks, pl.ds(0, dim)], w_sem.at[1, i]),
                pltpu.make_async_copy(wv_hbm.at[layer, ks], wkv_buf.at[ks, pl.ds(dim, dim)], w_sem.at[2, i]))

    load_k = pltpu.make_async_copy(k_hbm.at[layer], k_buf, in_sem.at[0])
    load_v = pltpu.make_async_copy(v_hbm.at[layer], v_buf, in_sem.at[1])
    load_x = pltpu.make_async_copy(x_ref, x_buf, in_sem.at[3])
    load_norm = pltpu.make_async_copy(norm_ref, norm_buf, in_sem.at[4])
    load_x.start()
    load_norm.start()
    for i in range(CHUNKS):
        for copy in load_weights(i):
            copy.start()
    load_k.start()
    load_v.start()

    load_x.wait()
    load_norm.wait()
    sum_sq = jnp.zeros((rows, 1), jnp.float32)
    for i in range(CHUNKS):
        part = x_buf[:, pl.ds(i * chunk, chunk)].astype(jnp.float32)
        sum_sq = sum_sq + jnp.sum(part * part, axis=-1, keepdims=True)
    scale = lax.rsqrt(sum_sq / width + 1e-5)
    for i in range(CHUNKS):
        cols = pl.ds(i * chunk, chunk)
        h_buf[:, cols] = (x_buf[:, cols].astype(jnp.float32) * scale * norm_buf[layer:layer + 1, cols].astype(jnp.float32)).astype(jnp.bfloat16)

    square = (rows, rows)
    diagonal = lax.broadcasted_iota(jnp.int32, square, 0) == lax.broadcasted_iota(jnp.int32, square, 1)
    column = jnp.sum(jnp.where(diagonal, jnp.broadcast_to(pos_ref[...].astype(jnp.float32), square), 0.0), axis=-1, keepdims=True)
    angles = column * freq_ref[...]
    lane = lax.broadcasted_iota(jnp.int32, (rows, dim), 1)
    cos_tab = jnp.cos(angles)
    sin_tab = jnp.where(lane < dim // 2, -jnp.sin(angles), jnp.sin(angles))

    for i in range(CHUNKS):
        for copy in load_weights(i):
            copy.wait()
        ks = pl.ds(i * chunk, chunk)
        q_part = jnp.dot(h_buf[:, ks], wq_buf[ks, :], preferred_element_type=jnp.float32)
        kv_part = jnp.dot(h_buf[:, ks], wkv_buf[ks, :], preferred_element_type=jnp.float32)
        if i == 0:
            q_buf[...] = q_part
            kv_buf[...] = kv_part
        else:
            q_buf[...] += q_part
            kv_buf[...] += kv_part

    def rounded(value):
        return value.astype(jnp.bfloat16).astype(jnp.float32)

    def rope(vec):
        vec = rounded(vec)
        half = dim // 2
        swapped = jnp.concatenate([vec[:, half:], vec[:, :half]], axis=-1)
        return rounded(vec * cos_tab + swapped * sin_tab)

    for j in range(heads):
        cols = pl.ds(j * dim, dim)
        q_buf[:, cols] = rope(q_buf[:, cols])
    kv_buf[:, pl.ds(0, dim)] = rope(kv_buf[:, pl.ds(0, dim)])
    kv_buf[:, pl.ds(dim, dim)] = rounded(kv_buf[:, pl.ds(dim, dim)])

    load_k.wait()
    load_v.wait()

    def store(g):
        part = pl.ds(pl.multiple_of(g * GROUP, GROUP), GROUP)
        return (pltpu.make_async_copy(k_buf.at[part], k_out.at[layer, part], out_sem.at[0, g]),
                pltpu.make_async_copy(v_buf.at[part], v_out.at[layer, part], out_sem.at[1, g]))

    def update(g, carry):
        base = pl.multiple_of(g * GROUP, GROUP)
        fresh = kv_buf[pl.ds(base, GROUP), :]
        for i in range(GROUP):
            pos = pos_smem[base + i]
            top = pl.multiple_of((pos // ROWS) * ROWS, ROWS)
            here = lax.broadcasted_iota(jnp.int32, (ROWS, dim), 0) == pos - top
            for buf, off in ((k_buf, 0), (v_buf, dim)):
                old = buf[base + i, pl.ds(top, ROWS), :].astype(jnp.float32)
                new = jnp.broadcast_to(fresh[i:i + 1, off:off + dim], (ROWS, dim))
                buf[base + i, pl.ds(top, ROWS), :] = jnp.where(here, new, old).astype(jnp.bfloat16)

        @pl.when(g > 0)
        def _():
            for copy in store(g - 1):
                copy.start()
        return carry

    lax.fori_loop(0, groups, update, 0)
    for copy in store(groups - 1):
        copy.start()

    request = lax.rem(lax.broadcasted_iota(jnp.int32, (heads * GROUP, 1), 0), GROUP)
    first_col = request * seq
    col = lax.broadcasted_iota(jnp.int32, (heads * GROUP, GROUP * seq), 1)

    def weigh(step, carry):
        done = []
        for k in range(TOGETHER):
            g = step * TOGETHER + k
            base = pl.multiple_of(g * GROUP, GROUP)
            block = pl.ds(base, GROUP)
            last_col = first_col
            for i in range(GROUP):
                last_col = jnp.where(request == i, i * seq + pos_smem[base + i], last_col)
            query = jnp.concatenate([q_buf[block, pl.ds(j * dim, dim)] for j in range(heads)], axis=0).astype(jnp.bfloat16)
            keys = k_buf[block].reshape(GROUP * seq, dim)
            scores = lax.dot_general(query, keys, (((1,), (1,)), ((), ())), preferred_element_type=jnp.float32) * (dim ** -0.5)
            scores = jnp.where((col >= first_col) & (col <= last_col), scores, -jnp.inf)
            weight = jnp.exp(scores - jnp.max(scores, axis=-1, keepdims=True))
            done.append((g, (weight * (1.0 / jnp.sum(weight, axis=-1, keepdims=True))).astype(jnp.bfloat16)))
        for g, prob in done:
            prob_buf[g] = prob
        return carry

    def mix(step, carry):
        done = []
        for k in range(TOGETHER):
            g = step * TOGETHER + k
            block = pl.ds(pl.multiple_of(g * GROUP, GROUP), GROUP)
            values = v_buf[block].reshape(GROUP * seq, dim)
            done.append((block, jnp.dot(prob_buf[g], values, preferred_element_type=jnp.float32)))
        for block, mixed in done:
            for j in range(heads):
                mix_buf[block, pl.ds(j * dim, dim)] = mixed[j * GROUP:(j + 1) * GROUP]
        return carry

    lax.fori_loop(0, groups // TOGETHER, weigh, 0)
    lax.fori_loop(0, groups // TOGETHER, mix, 0)
    att_buf[...] = mix_buf[...].astype(jnp.bfloat16)
    store_out = pltpu.make_async_copy(att_buf, out_ref, in_sem.at[2])
    store_out.start()

    def drain(g, carry):
        for copy in store(g):
            copy.wait()
        return carry

    lax.fori_loop(0, groups, drain, 0)
    store_out.wait()


CHUNKS = 2
GROUP = 8
ROWS = 16
TOGETHER = 16


def attention_call(layer, x, norm, positions, freqs, w_query, w_key, w_value, k_cache, v_cache, k_done, v_done):
    rows, width = x.shape
    inner = w_query.shape[2]
    seq, dim = k_cache.shape[2], k_cache.shape[3]
    bf16 = jnp.bfloat16
    first = k_done is None
    vmem = pl.BlockSpec(memory_space=pltpu.VMEM)
    hbm = pl.BlockSpec(memory_space=pltpu.HBM)
    smem = pl.BlockSpec(memory_space=pltpu.SMEM)
    args = [x, norm, positions, positions[None, :], freqs, w_query, w_key, w_value, k_cache, v_cache]
    specs = [hbm, hbm, smem, vmem, vmem, hbm, hbm, hbm, hbm, hbm]
    aliases = {}
    if not first:
        aliases = {len(args): 1, len(args) + 1: 2}
        args += [k_done, v_done]
        specs += [hbm, hbm]
    weights = width * (inner + 2 * dim)
    return pl.pallas_call(
        functools.partial(attention_kernel, layer, first),
        out_shape=[jax.ShapeDtypeStruct((rows, inner), bf16), jax.ShapeDtypeStruct(k_cache.shape, bf16), jax.ShapeDtypeStruct(v_cache.shape, bf16)],
        in_specs=specs,
        out_specs=[hbm, hbm, hbm],
        scratch_shapes=[
            pltpu.VMEM((width, inner), bf16),
            pltpu.VMEM((width, 2 * dim), bf16),
            pltpu.VMEM((rows, seq, dim), bf16),
            pltpu.VMEM((rows, seq, dim), bf16),
            pltpu.VMEM((rows, width), bf16),
            pltpu.VMEM((rows, inner), jnp.float32),
            pltpu.VMEM((rows, 2 * dim), jnp.float32),
            pltpu.VMEM((rows, inner), jnp.float32),
            pltpu.VMEM((rows // GROUP, GROUP * inner // dim, GROUP * seq), bf16),
            pltpu.VMEM((rows, inner), bf16),
            pltpu.VMEM((rows, width), bf16),
            pltpu.VMEM(norm.shape, bf16),
            pltpu.SemaphoreType.DMA((3, CHUNKS)),
            pltpu.SemaphoreType.DMA((5,)),
            pltpu.SemaphoreType.DMA((2, rows // GROUP)),
        ],
        input_output_aliases=aliases,
        compiler_params=pltpu.CompilerParams(vmem_limit_bytes=67043328),
        cost_estimate=pl.CostEstimate(flops=2 * rows * weights, bytes_accessed=2 * weights, transcendentals=rows * seq),
        name='attention_layer',
    )(*args)


PIECES = 5
RELAYED = 4
TILE = 256


def mlp_kernel(layer, chips, attn_hbm, res_ref, norm_hbm, wo_hbm, wg_hbm, wu_hbm, wd_hbm, out_ref,
               o_buf, g_buf, u_buf, d_buf, full, part, act, res, attn_ref, norm_ref, swap_in, summed, owner_in,
               w_sem, io_sem, rs_send, rs_recv, ag_send, ag_recv):
    rows, width = full.shape
    piece = width // PIECES
    half_rows = rows // 2
    own_rows = half_rows // chips
    me = lax.axis_index('tp')
    core = lax.rem(me, 2)
    chip = me // 2
    partner = me + 1 - 2 * core
    peers = [2 * lax.rem(chip + hop, chips) + core for hop in range(chips)]
    hops = tuple(sorted(range(1, chips), key=lambda hop: -min(hop, chips - hop)))
    nearest = hops[::-1]
    far = chips // 2
    n_gate = g_buf.shape[0]

    def piece_cols(p):
        return pl.ds(p * piece, piece)

    def rows_of(offset):
        return pl.ds(pl.multiple_of(core * half_rows + lax.rem(chip + offset, chips) * own_rows, own_rows), own_rows)

    def block(offset):
        return pl.ds(pl.multiple_of(lax.rem(chip + offset, chips) * own_rows, own_rows), own_rows)

    mine = rows_of(0)
    other_rows = pl.ds(pl.multiple_of((1 - core) * half_rows, half_rows), half_rows)
    my_rows = pl.ds(pl.multiple_of(core * half_rows, half_rows), half_rows)

    def load_out(p):
        return pltpu.make_async_copy(wo_hbm.at[layer, :, piece_cols(p)], o_buf.at[p], w_sem.at[p])

    def load_down(p):
        return pltpu.make_async_copy(wd_hbm.at[layer, :, piece_cols(p)], d_buf.at[p], w_sem.at[PIECES + p])

    def load_gate(j):
        cols = pl.ds(pl.multiple_of(j * TILE, TILE), TILE)
        return pltpu.make_async_copy(wg_hbm.at[layer, :, cols], g_buf.at[j], w_sem.at[2 * PIECES + j])

    def load_up(j):
        cols = pl.ds(pl.multiple_of(j * TILE, TILE), TILE)
        return pltpu.make_async_copy(wu_hbm.at[layer, :, cols], u_buf.at[j], w_sem.at[2 * PIECES + n_gate + j])

    load_res = pltpu.make_async_copy(res_ref.at[mine], res, io_sem.at[0])
    load_attn = pltpu.make_async_copy(attn_hbm, attn_ref, io_sem.at[1 + PIECES])
    load_norm = pltpu.make_async_copy(norm_hbm, norm_ref, io_sem.at[2 + PIECES])

    def store(p):
        return pltpu.make_async_copy(full.at[:, piece_cols(p)], out_ref.at[:, piece_cols(p)], io_sem.at[1 + p])

    load_attn.start()
    load_out(0).start()
    load_res.start()
    load_norm.start()

    def start_gate_up():
        for j in range(n_gate):
            load_gate(j).start()
            load_up(j).start()

    def start_down():
        for p in range(PIECES):
            load_down(p).start()

    barrier = pltpu.get_barrier_semaphore()
    for peer in [partner] + peers[1:]:
        pl.semaphore_signal(barrier, inc=1, device_id={'tp': peer}, device_id_type=pl.DeviceIdType.MESH)
    pl.semaphore_wait(barrier, chips)
    for p in range(1, PIECES):
        load_out(p).start()

    def remote(src, dst, send_sem, recv_sem, peer):
        return pltpu.make_async_remote_copy(src_ref=src, dst_ref=dst, send_sem=send_sem, recv_sem=recv_sem, device_id={'tp': peer}, device_id_type=pl.DeviceIdType.MESH)

    def swap(p):
        return remote(part.at[other_rows, piece_cols(p)], swap_in.at[p], rs_send.at[0, p], rs_recv.at[0, p], partner)

    def to_owner(p, hop):
        return remote(summed.at[p, block(hop)], owner_in.at[hop - 1, p], rs_send.at[hop, p], rs_recv.at[hop, p], peers[hop])

    def spread(p, hop):
        sems = ag_send.at[hop, p], ag_recv.at[hop, p]
        if hop == far and p < RELAYED:
            landed = full.at[rows_of(chips - 1 if p % 2 == 0 else 1), piece_cols(p)]
            return remote(landed, landed, *sems, peers[1 if p % 2 == 0 else chips - 1])
        return remote(res.at[:, piece_cols(p)], full.at[mine, piece_cols(p)], *sems, peers[hop] if hop else partner)

    def forward(p, hop):
        landed = full.at[rows_of(chips - hop), piece_cols(p)]
        return remote(landed, landed, ag_send.at[chips + hop - 1, p], ag_recv.at[chips + hop - 1, p], partner)

    def add_over_tp(lhs_ref, w_buf, load, after_products, after_sums):
        def product(p):
            load(p).wait()
            for i in range(piece // TILE):
                part[:, pl.ds(p * piece + i * TILE, TILE)] = jnp.dot(
                    lhs_ref[...], w_buf[p, :, pl.ds(i * TILE, TILE)], preferred_element_type=jnp.float32).astype(jnp.bfloat16)
            swap(p).start()

        def chip_sum(p):
            swap(p).wait_recv()
            summed[p] = (part[my_rows, piece_cols(p)].astype(jnp.float32) + swap_in[p].astype(jnp.float32)).astype(jnp.bfloat16)
            for hop in hops:
                to_owner(p, hop).start()

        product(0)
        for p in range(1, PIECES):
            product(p)
            chip_sum(p - 1)
        after_products()
        chip_sum(PIECES - 1)
        after_sums()
        for p in range(PIECES):
            total = summed[p, block(0)].astype(jnp.float32)
            for hop in range(1, chips):
                to_owner(p, hop).wait_recv()
                total = total + owner_in[hop - 1, p].astype(jnp.float32)
            new = res[:, piece_cols(p)].astype(jnp.float32) + total.astype(jnp.bfloat16).astype(jnp.float32)
            new = new.astype(jnp.bfloat16)
            res[:, piece_cols(p)] = new
            full[mine, piece_cols(p)] = new
            for hop in hops + (0,):
                if hop != far or p >= RELAYED:
                    spread(p, hop).start()
        for p in range(PIECES):
            for hop in nearest[:-1]:
                spread(p, hop).wait_recv()
                if p < RELAYED and hop == (1 if p % 2 == 0 else chips - 1):
                    spread(p, far).start()
                forward(p, hop).start()
        for p in range(PIECES):
            spread(p, far).wait_recv()
            forward(p, far).start()

    def gathered(p):
        spread(p, 0).wait_recv()
        for hop in nearest:
            forward(p, hop).wait_recv()

    def drain_sends():
        for p in range(PIECES):
            swap(p).wait_send()
            for hop in range(1, chips):
                to_owner(p, hop).wait_send()
                forward(p, hop).wait_send()
            for hop in range(chips):
                spread(p, hop).wait_send()

    load_attn.wait()
    load_res.wait()
    load_norm.wait()
    add_over_tp(attn_ref, o_buf, load_out, start_gate_up, start_down)
    sum_sq = jnp.zeros((rows, 1), jnp.float32)
    for p in range(PIECES):
        gathered(p)
        new = full[:, piece_cols(p)].astype(jnp.float32)
        sum_sq = sum_sq + jnp.sum(new * new, axis=-1, keepdims=True)
    drain_sends()
    scale = lax.rsqrt(sum_sq / width + 1e-5)
    for p in range(PIECES):
        cols = piece_cols(p)
        part[:, cols] = (full[:, cols].astype(jnp.float32) * scale * norm_ref[layer:layer + 1, cols].astype(jnp.float32)).astype(jnp.bfloat16)

    def gate_up(j, carry):
        load_gate(j).wait()
        load_up(j).wait()
        gate = jnp.dot(part[...], g_buf[j], preferred_element_type=jnp.float32).astype(jnp.bfloat16).astype(jnp.float32)
        up = jnp.dot(part[...], u_buf[j], preferred_element_type=jnp.float32).astype(jnp.bfloat16).astype(jnp.float32)
        act[:, pl.ds(pl.multiple_of(j * TILE, TILE), TILE)] = (gate * jax.nn.sigmoid(gate) * up).astype(jnp.bfloat16)
        return carry

    lax.fori_loop(0, n_gate, gate_up, 0)
    add_over_tp(act, d_buf, load_down, lambda: None, lambda: None)
    for p in range(PIECES):
        gathered(p)
        store(p).start()
    drain_sends()
    for p in range(PIECES):
        store(p).wait()


def mlp_call(layer, chips, attended, hidden, norm, w_out, w_gate, w_up, w_down):
    rows, inner = attended.shape
    width = w_gate.shape[1]
    ff = w_gate.shape[2]
    piece = width // PIECES
    own_rows = rows // 2 // chips
    bf16 = jnp.bfloat16
    hbm = pl.BlockSpec(memory_space=pltpu.HBM)
    scratch = [
        pltpu.VMEM((PIECES, inner, piece), bf16),
        pltpu.VMEM((ff // TILE, width, TILE), bf16),
        pltpu.VMEM((ff // TILE, width, TILE), bf16),
        pltpu.VMEM((PIECES, ff, piece), bf16),
        pltpu.VMEM((rows, width), bf16),
        pltpu.VMEM((rows, width), bf16),
        pltpu.VMEM((rows, ff), bf16),
        pltpu.VMEM((own_rows, width), bf16),
        pltpu.VMEM((rows, inner), bf16),
        pltpu.VMEM(norm.shape, bf16),
        pltpu.VMEM((PIECES, rows // 2, piece), bf16),
        pltpu.VMEM((PIECES, rows // 2, piece), bf16),
        pltpu.VMEM((chips - 1, PIECES, own_rows, piece), bf16),
        pltpu.SemaphoreType.DMA((2 * PIECES + 2 * (ff // TILE),)),
        pltpu.SemaphoreType.DMA((3 + PIECES,)),
        pltpu.SemaphoreType.DMA((chips, PIECES)),
        pltpu.SemaphoreType.DMA((chips, PIECES)),
        pltpu.SemaphoreType.DMA((2 * chips - 1, PIECES)),
        pltpu.SemaphoreType.DMA((2 * chips - 1, PIECES)),
    ]
    weights = inner * width + 3 * width * ff
    return pl.pallas_call(
        functools.partial(mlp_kernel, layer, chips),
        out_shape=jax.ShapeDtypeStruct((rows, width), bf16),
        in_specs=[hbm] * 7,
        out_specs=hbm,
        scratch_shapes=scratch,
        compiler_params=pltpu.CompilerParams(collective_id=layer, has_side_effects=True, vmem_limit_bytes=67043328),
        cost_estimate=pl.CostEstimate(flops=2 * rows * weights, bytes_accessed=2 * weights, transcendentals=rows * ff),
        name='mlp_layer',
    )(attended, hidden, norm, w_out, w_gate, w_up, w_down)


def solution(mesh):
    row_spec = P('dp', None)
    pos_spec = P('dp')
    cache_spec = P(None, 'dp', None, 'tp', None)
    norm_spec = P(None, None)
    col_spec = P(None, None, 'tp')
    split_rows = P(None, 'tp', None)
    chips = mesh.shape['tp'] // 2

    def local_step(hidden, positions, k_cache, v_cache, attn_norm, w_query, w_key, w_value, w_out, mlp_norm, w_gate, w_up, w_down):
        layers, batch, seq, kv_heads, dim = k_cache.shape
        freqs = rope_freqs(dim)
        k_old = k_cache.reshape(layers, batch, seq, dim)
        v_old = v_cache.reshape(layers, batch, seq, dim)
        k_out = v_out = None
        for layer in range(layers):
            attended, k_out, v_out = attention_call(layer, hidden, attn_norm, positions, freqs, w_query, w_key, w_value, k_old, v_old, k_out, v_out)
            hidden = mlp_call(layer, chips, attended, hidden, mlp_norm, w_out, w_gate, w_up, w_down)
        shape = (layers, batch, seq, kv_heads, dim)
        return hidden, k_out.reshape(shape), v_out.reshape(shape)

    return jax.shard_map(local_step, mesh=mesh, in_specs=(row_spec, pos_spec, cache_spec, cache_spec, norm_spec, col_spec, col_spec, col_spec, split_rows, norm_spec, col_spec, col_spec, split_rows), out_specs=(row_spec, cache_spec, cache_spec), check_vma=False)
```
